32 devices in a mesh: member: 8 (over z, core), space: 4 (over y, x).
Axes of the slice: x: 2, y: 2, z: 4, core: 2. Of those that a mesh axis runs over, the one named last changes fastest.
Arguments:
- weather: bfloat16 [8, 84, 64, 1440], P('member', None, 'space'), may hold values from -6 to 6
- coefficients: int32 [8, 84, 2, 364, 361], P('member', None, None, 'space'), may hold values from -1073741824 to 1073741823
- channel_scale: float32 [84], replicated, may hold values from 0.3 to 3
Outputs:
- perturbed: bfloat16 [8, 84, 64, 1440], P('member', None, 'space')
The draws below stay inside these ranges and needn't reach their ends.
All inputs are finite; a program needn't handle non-finite values.
Results may differ from the reference program's by a relative error of at most 0.007.
Values may be sent and summed in bfloat16 or wider, within the bound.
A program may use at most 192 MiB of HBM per device.

```python
import math
import jax
import jax.numpy as jnp
from jax import lax

CH = 84
LON = 1440
E = 8
LAT = 64
LAT0 = 328
LP = 361
MP = 364


def with_ends(values, rng, low, largest):
    longest = values.shape.index(max(values.shape))
    spots = []
    for shift in (0, 1):
        where = [jax.random.randint(jax.random.fold_in(rng, axis), (), 0, length) for axis, length in enumerate(values.shape)]
        where[longest] = (where[longest] + shift) % values.shape[longest]
        spots.append(tuple(where))
    return values.at[spots[0]].set(low).at[spots[1]].set(largest)


def shard_levels(key, extent, pieces, least, high):
    level = 1.0
    for position, blocks in pieces:
        heights = jax.random.uniform(jax.random.fold_in(jax.random.fold_in(key, 6), position), (blocks,), jnp.float32, least / len(pieces), high / len(pieces))
        level = level * jnp.repeat(jnp.exp(heights), extent[position] // blocks).reshape((-1,) + (1,) * (len(extent) - 1 - position))
    return level


def normal_values(own_key, dims, spread, reach, shards=(), kind=jnp.bfloat16):
    loudness = shard_levels(own_key, dims, shards, -0.22, 0.18) if shards else 1.0
    values = jax.random.normal(own_key, dims, jnp.float32) * spread * loudness
    return jnp.minimum(jnp.maximum(values, -reach), reach).astype(kind)


def setup_inputs(seed: int = 0) -> dict:
    key_list = jax.random.split(jax.random.key(seed), 4)
    weather = normal_values(key_list[0], (E, CH, LAT, LON), 1.0, 6.0, ((0, 8), (2, 4)))
    coefficients = with_ends(jax.random.randint(key_list[1], (E, CH, 2, MP, LP), -1073741824, 1073741824), jax.random.fold_in(key_list[1], 1), -1073741824, 1073741823).astype(jnp.int32)
    channel_scale = jnp.clip(jnp.exp(jax.random.uniform(key_list[2], (CH,), jnp.float32, math.log(0.3), math.log(3.0))), 0.3, 3.0)
    return dict(weather=weather, coefficients=coefficients, channel_scale=channel_scale)


def diagonal_log(order_count):
    steps_up = jnp.arange(1, order_count, dtype=jnp.int32).astype(jnp.float32)
    terms = 0.5 * jnp.log((2.0 * steps_up + 1.0) / (2.0 * steps_up))
    return jnp.concatenate([jnp.zeros((1,), jnp.float32), jnp.cumsum(terms)])

def legendre_table(orders, colatitude, order_logs, degree_count):
    order_values = orders.astype(jnp.float32)[:, None]
    cosine = jnp.cos(colatitude)[None, :]
    sine_values = jnp.sin(colatitude)[None, :]
    diagonal = jnp.exp(order_logs[:, None] - 0.5 * math.log(4.0 * math.pi) + order_values * jnp.log(sine_values))
    block_size = 16
    turn_count = (degree_count + block_size - 1) // block_size
    order_square = order_values * order_values

    def advance(carry, turn_index):
        older_row, newer_row = carry
        produced = []
        for inner_step in range(block_size):
            degree = (turn_index * block_size + inner_step).astype(jnp.float32)
            degree_square = degree * degree
            prior = degree - 1.0
            factor_up = jnp.sqrt(jnp.maximum(4.0 * degree_square - 1.0, 1.0) / jnp.maximum(degree_square - order_square, 1.0))
            factor_down = jnp.sqrt(jnp.maximum(prior * prior - order_square, 0.0) / jnp.maximum(4.0 * prior * prior - 1.0, 1.0))
            next_row = factor_up * (cosine * newer_row - factor_down * older_row)
            next_row = jnp.where(degree < order_values, 0.0, jnp.where(degree == order_values, diagonal, next_row))
            produced.append(next_row)
            older_row, newer_row = (newer_row, next_row)
        return ((older_row, newer_row), jnp.stack(produced))
    empty = jnp.zeros_like(diagonal)
    carried, stacked = lax.scan(advance, (empty, empty), jnp.arange(turn_count, dtype=jnp.int32))
    return stacked.reshape(turn_count * block_size, orders.shape[0], colatitude.shape[0])[:degree_count]

def spectral_values(coefficients, orders):
    degree_count = coefficients.shape[-1]
    degrees = jnp.arange(degree_count, dtype=jnp.int32)
    keep = degrees[None, :] >= orders[:, None]
    factor = math.sqrt(3.0) * math.sqrt(4.0 * math.pi) / degree_count * 2.0 ** (-30)
    values = coefficients.astype(jnp.float32) * factor
    return jnp.where(keep, values, 0.0).astype(jnp.bfloat16)

def fourier_basis(order_count, lon_count):
    orders = jnp.arange(order_count, dtype=jnp.int32)
    columns = jnp.arange(lon_count, dtype=jnp.int32)
    phases = orders[:, None] * columns[None, :] % lon_count
    angles = 2.0 * math.pi / lon_count * phases.astype(jnp.float32)
    weights = jnp.where(orders == 0, 1.0, math.sqrt(2.0)).astype(jnp.float32)[:, None]
    return jnp.stack([weights * jnp.cos(angles), weights * jnp.sin(angles)]).astype(jnp.bfloat16)

def reference(weather, coefficients, channel_scale):
    orders = jnp.arange(MP, dtype=jnp.int32)
    colatitude = math.pi * (LAT0 + jnp.arange(LAT, dtype=jnp.int32)).astype(jnp.float32) / (LON // 2)
    legendre = legendre_table(orders, colatitude, diagonal_log(MP), LP).astype(jnp.bfloat16)
    legendre_wide = lax.optimization_barrier(legendre).astype(jnp.float32)
    basis = fourier_basis(MP, LON).reshape(2 * MP, LON)

    def one_member(coef_member):
        spectral = lax.optimization_barrier(spectral_values(coef_member, orders)).astype(jnp.float32)
        fourier = jnp.einsum('cpml,lmt->ctpm', spectral, legendre_wide, precision=lax.Precision.HIGHEST).astype(jnp.bfloat16)
        noise = jnp.dot(fourier.reshape(CH * LAT, 2 * MP), basis, preferred_element_type=jnp.float32)
        return noise.astype(jnp.bfloat16).reshape(CH, LAT, LON)
    noise_all = lax.map(one_member, coefficients)

    def add_up(total, noise_member):
        return (total + noise_member.astype(jnp.float32), None)
    total, unused = lax.scan(add_up, jnp.zeros((CH, LAT, LON), jnp.float32), noise_all)
    mean = total / E

    def perturb(pair):
        weather_member, noise_member = pair
        centred = noise_member.astype(jnp.float32) - mean
        return (weather_member.astype(jnp.float32) + channel_scale[:, None, None] * centred).astype(jnp.bfloat16)
    return lax.map(perturb, (weather, noise_all))
```

```python
import functools
import math

import jax
import jax.numpy as jnp
from jax import lax
from jax.experimental import pallas as pl
from jax.experimental.pallas import tpu as pltpu
from jax.sharding import PartitionSpec as P


def round_up(value, step):
    return (value + step - 1) // step * step


def diagonal_log(order_count):
    steps_up = jnp.arange(1, order_count, dtype=jnp.int32).astype(jnp.float32)
    terms = 0.5 * jnp.log((2.0 * steps_up + 1.0) / (2.0 * steps_up))
    return jnp.concatenate([jnp.zeros((1,), jnp.float32), jnp.cumsum(terms)])


def synthesis_kernel(
    block, lat, order_ref, cosine_ref, diagonal_ref, coef, out_ref, table, kept, held, arrived
):
    half, lanes = order_ref.shape
    channels, order_local, _, degree_count = coef.shape
    rows = held.shape[1]
    both = 2 * rows
    degrees = round_up(degree_count, 8)
    pitch = degrees + 8
    factor = math.sqrt(3.0) * math.sqrt(4.0 * math.pi) / degree_count * 2.0 ** (-30)
    turn = pl.program_id(0)

    def fetch(step, act):
        base = lax.rem(step, 2) * (2 * block)
        for spot in range(2 * block):
            slot = step * block + spot % block + spot // block * half
            slot = jnp.minimum(slot, order_local - 1)
            copy = pltpu.make_async_copy(
                coef.at[:, slot], held.at[base + spot, pl.ds(0, channels)], arrived.at[base + spot]
            )
            act(copy)

    @pl.when(turn == 0)
    def begin():
        fetch(turn, lambda copy: copy.start())

    @pl.when(turn + 1 < pl.num_programs(0))
    def ahead():
        fetch(turn + 1, lambda copy: copy.start())

    @pl.when(pl.program_id(0) == 0)
    def build():
        order = order_ref[...]
        order_square = order * order
        cosine = jnp.broadcast_to(cosine_ref[...], (half, lanes))
        diagonal = diagonal_ref[...]

        def advance(step, carry):
            older, newer, down = carry
            degree = step.astype(jnp.float32)
            wide = jnp.full((half, lanes), degree, jnp.float32)
            square = wide * wide
            ratio = jnp.maximum(square - order_square, 0.25) / jnp.maximum(4.0 * square - 1.0, 1.0)
            up = lax.rsqrt(ratio)
            row = up * (cosine * newer - down * older)
            row = jnp.where(wide < order, 0.0, jnp.where(wide == order, diagonal, row))
            for tile in range(lanes // 128):
                table[pl.ds(tile * half * pitch + step, half, stride=pitch), :] = row[
                    :, tile * 128 : tile * 128 + 128
                ]
            return newer, row, ratio * up

        zero = order * 0.0
        lax.fori_loop(0, degrees, advance, (zero, zero, zero), unroll=4)

    fetch(turn, lambda copy: copy.wait())
    first = turn * block
    low = lax.broadcasted_iota(jnp.int32, (both, lanes), 1) < lanes // 2
    pack = 128 // lat
    bands = lanes // 2 // lat
    groups = out_ref.shape[0]
    deep = half + 8

    def read(spot):
        values = held[lax.rem(turn, 2) * (2 * block) + spot].astype(jnp.float32) * factor
        return values.reshape(both, degree_count).astype(jnp.bfloat16)

    for inner in range(block):
        columns = []
        for tile in range(lanes // 128):
            start = pl.multiple_of((tile * half + first + inner) * pitch, 8)
            columns.append(table[pl.ds(start, degrees), :].astype(jnp.bfloat16))
        values = jnp.concatenate(columns, axis=1)[:degree_count]
        stacked = jnp.concatenate([read(inner), read(inner + block)], axis=0)
        found = jnp.dot(stacked, values, preferred_element_type=jnp.float32)
        merged = jnp.where(low, found[:both], found[both:])
        for tile in range(lanes // 128):
            start = tile * both * deep + first + inner
            kept[pl.ds(start, both, stride=deep), :] = merged[:, tile * 128 : tile * 128 + 128]

    @pl.when(pl.program_id(0) == pl.num_programs(0) - 1)
    def regroup():
        chunk = lax.broadcasted_iota(jnp.int32, (half, 128), 1) // lat
        for tile in range(lanes // 128):
            def one_group(group, carry):
                for part in range(2):
                    planes = []
                    for spot in range(pack):
                        row = tile * both + (group * pack + spot) * 2 + part
                        planes.append(kept[pl.ds(pl.multiple_of(row * deep, 8), half), :])
                    gap = 1
                    while gap < pack:
                        upper = (chunk // gap) % 2 == 1
                        for spot in range(pack):
                            if (spot // gap) % 2 == 0:
                                one, two = planes[spot], planes[spot + gap]
                                planes[spot] = jnp.where(upper, pltpu.roll(two, gap * lat, 1), one)
                                planes[spot + gap] = jnp.where(
                                    upper, two, pltpu.roll(one, 128 - gap * lat, 1)
                                )
                        gap *= 2
                    for spot in range(pack):
                        high, band = divmod(tile * pack + spot, bands)
                        out_ref[group, band, high, part] = planes[spot].astype(jnp.bfloat16)
                return carry

            lax.fori_loop(0, groups, one_group, 0)


def synthesize(coefficients, order_plane, cosine_row, diagonal_plane, lat):
    channels, _, _, degree_count = coefficients.shape
    half, lanes = order_plane.shape
    block = 8
    rows = round_up(channels, 128 // lat)
    out_dims = (rows * lat // 128, lanes // 2 // lat, 2, 2, half, 128)
    return pl.pallas_call(
        functools.partial(synthesis_kernel, block, lat),
        grid=(half // block,),
        out_shape=jax.ShapeDtypeStruct(out_dims, jnp.bfloat16),
        in_specs=[
            pl.BlockSpec((half, lanes), lambda i: (0, 0)),
            pl.BlockSpec((1, lanes), lambda i: (0, 0)),
            pl.BlockSpec((half, lanes), lambda i: (0, 0)),
            pl.BlockSpec(memory_space=pl.ANY),
        ],
        out_specs=pl.BlockSpec(out_dims, lambda i: (0, 0, 0, 0, 0, 0)),
        scratch_shapes=[
            pltpu.VMEM((lanes // 128 * half * (round_up(degree_count, 8) + 8), 128), jnp.float32),
            pltpu.VMEM((lanes // 128 * 2 * rows * (half + 8), 128), jnp.float32),
            pltpu.VMEM((4 * block, rows, 2, degree_count), jnp.int32),
            pltpu.SemaphoreType.DMA((4 * block,)),
        ],
        compiler_params=pltpu.CompilerParams(vmem_limit_bytes=60 * 1024 * 1024),
    )(order_plane, cosine_row, diagonal_plane, coefficients)


def quarter_waves(turns):
    quarter = turns * 4.0
    nearest = jnp.floor(quarter + 0.5)
    angle = (quarter - nearest) * (0.5 * math.pi)
    square = angle * angle
    sine = cosine = None
    for power in (8, 6, 4, 2, 0):
        even = (-1.0) ** (power // 2) / math.factorial(power)
        odd = (-1.0) ** (power // 2) / math.factorial(power + 1)
        cosine = even + (0.0 if cosine is None else cosine * square)
        sine = odd + (0.0 if sine is None else sine * square)
    sine = sine * angle
    half_turns = jnp.floor(nearest * 0.5)
    swap = nearest - 2.0 * half_turns > 0.5
    flip = 1.0 - 2.0 * (half_turns - 2.0 * jnp.floor(half_turns * 0.5))
    one = jnp.where(swap, -sine, cosine) * flip
    two = jnp.where(swap, cosine, sine) * flip
    return one, two


def exchange_kernel(
    order_local, sent, weather, scale, out, raw, near, sums, lower, other, total, basis, field,
    turned, field_in, field_out, *sems
):
    a2a_send, a2a_recv = sems[0], sems[1]
    pair = {
        "near": (sems[2], sems[3]),
        "line": (sems[4], sems[5]),
        "swap": (sems[6], sems[7]),
        "back": (sems[8], sems[9]),
        "mate": (sems[10], sems[11]),
    }
    parts, bands, depth, _ = sent.shape
    flat, lon_count = weather.shape
    channels = scale.shape[0]
    lat = flat // channels
    member_count = lax.axis_size("member")
    chips = member_count // 2
    middle = chips // 2
    me = lax.axis_index("member")
    space = lax.axis_index("space")
    core = lax.rem(me, 2)
    chip = me // 2
    mate = chip * 2 + 1 - core
    left = chip < middle
    rank = jnp.where(left, chip, chips - 1 - chip)
    inward = jnp.where(left, chip + 1, chip - 1) * 2 + core
    outward = jnp.where(left, chip - 1, chip + 1) * 2 + core
    split = bands // 2
    mesh_ids = pl.DeviceIdType.MESH

    def spread(k, hop):
        target = lax.rem(space + hop, bands)
        return pltpu.make_async_remote_copy(
            src_ref=sent.at[k, target],
            dst_ref=raw.at[k, space],
            send_sem=a2a_send.at[k, hop],
            recv_sem=a2a_recv.at[k, hop],
            device_id={"space": target},
            device_id_type=mesh_ids,
        )

    def hand(kind, k, source, landing, target):
        return pltpu.make_async_remote_copy(
            src_ref=source,
            dst_ref=landing,
            send_sem=pair[kind][0].at[k],
            recv_sem=pair[kind][1].at[k],
            device_id={"member": target},
            device_id_type=mesh_ids,
        )

    def near_copy(k):
        return hand("near", k, raw.at[k, pl.ds((1 - core) * split, split)], near.at[k], mate)

    def line_copy(k):
        return hand("line", k, sums.at[k], lower.at[k], inward)

    def swap_copy(k):
        return hand("swap", k, sums.at[k], other.at[k], inward)

    def back_copy(k):
        return hand("back", k, total.at[k, core], total.at[k, core], outward)

    def mate_copy(k):
        return hand("mate", k, total.at[k, core], total.at[k, core], mate)

    def write_rows(k, count):
        rows = pl.ds(k * 128, count)
        return pltpu.make_async_copy(field.at[rows], out.at[rows], field_out.at[k])

    def stage_near(k):
        raw[k, space] = sent[k, space]
        for hop in range(1, bands):
            spread(k, hop).wait_recv()
        near_copy(k).start()

    def send_inward(k, level):
        @pl.when(rank == level)
        def _():
            if level == middle - 1:
                swap_copy(k).start()
            else:
                line_copy(k).start()

    def stage_sum(k):
        near_copy(k).wait_recv()
        mine = raw[k, pl.ds(core * split, split)].astype(jnp.float32) + near[k].astype(jnp.float32)
        sums[k] = mine.astype(jnp.bfloat16)
        send_inward(k, 0)

    def stage_line(level, k):
        @pl.when(rank == level)
        def _():
            line_copy(k).wait_recv()
            both = sums[k].astype(jnp.float32) + lower[k].astype(jnp.float32)
            sums[k] = both.astype(jnp.bfloat16)

        send_inward(k, level)

    def send_outward(k, level):
        if level > 0:
            back_copy(k).start()
        mate_copy(k).start()

    def stage_swap(k):
        @pl.when(rank == middle - 1)
        def _():
            swap_copy(k).wait_recv()
            both = sums[k].astype(jnp.float32) + other[k].astype(jnp.float32)
            total[k, core] = both.astype(jnp.bfloat16)
            send_outward(k, middle - 1)

    def stage_back(level, k):
        @pl.when(rank == level)
        def _():
            back_copy(k).wait_recv()
            send_outward(k, level)

    def stage_out(k):
        mate_copy(k).wait_recv()
        for band in range(bands):
            mean = total[k, band // split, band % split].astype(jnp.float32) * (1.0 / member_count)
            centred = raw[k, band].astype(jnp.float32) - mean
            turned[:, band * depth : (band + 1) * depth] = centred.T.astype(jnp.bfloat16)
        for start in range(0, lon_count, 256):
            width = min(256, lon_count - start)
            noise = jnp.dot(
                turned[...],
                basis[:, start : start + width],
                preferred_element_type=jnp.float32,
            )
            for step in range(128 // lat):
                amount = scale[jnp.minimum(k * (128 // lat) + step, channels - 1)]
                rows = pl.ds(pl.multiple_of(k * 128 + step * lat, lat), lat)
                state = field[rows, start : start + width].astype(jnp.float32)
                state = state + amount * noise[step * lat : (step + 1) * lat]
                field[rows, start : start + width] = state.astype(jnp.bfloat16)

        @pl.when(k < parts - 1)
        def _():
            write_rows(k, 128).start()

        @pl.when(k == parts - 1)
        def _():
            write_rows(parts - 1, flat - (parts - 1) * 128).start()

    stages = [stage_near, stage_sum]
    stages += [functools.partial(stage_line, level) for level in range(1, middle)]
    stages += [stage_swap]
    stages += [functools.partial(stage_back, level) for level in range(middle - 2, -1, -1)]
    stages += [stage_out]

    for k in range(parts):
        for hop in range(1, bands):
            spread(k, hop).start()
    load = pltpu.make_async_copy(weather, field.at[pl.ds(0, flat)], field_in.at[0])
    load.start()

    half = depth // 4
    lane = lax.broadcasted_iota(jnp.int32, (half, 128), 1).astype(jnp.float32)
    row = lax.broadcasted_iota(jnp.int32, (half, 128), 0).astype(jnp.float32)

    def turns(product):
        rest = product - jnp.floor(product * (1.0 / lon_count)) * lon_count
        rest = jnp.where(rest < 0.0, rest + lon_count, rest)
        rest = jnp.where(rest >= lon_count, rest - lon_count, rest)
        return rest * (1.0 / lon_count)

    def build(index, carry):
        band, high = index // 2, lax.rem(index, 2)
        slot = row + (high * half).astype(jnp.float32)
        order = slot + (band * order_local).astype(jnp.float32)
        weight = jnp.where(order < 0.5, 1.0, math.sqrt(2.0))
        weight = jnp.where(slot < order_local, weight, 0.0)
        real, imag = quarter_waves(turns(order * lane))
        real, imag = weight * real, weight * imag
        turn_real, turn_imag = quarter_waves(turns(order * 128.0))
        first = pl.multiple_of(band * depth + high * (2 * half), half)
        for start in range(0, lon_count, 128):
            width = min(128, lon_count - start)
            basis[pl.ds(first, half), start : start + width] = real[:, :width].astype(jnp.bfloat16)
            basis[pl.ds(first + half, half), start : start + width] = imag[:, :width].astype(
                jnp.bfloat16
            )
            real, imag = real * turn_real - imag * turn_imag, imag * turn_real + real * turn_imag
        return carry

    lax.fori_loop(0, 2 * bands, build, 0)
    load.wait()

    def advance(turn, carry):
        for place in reversed(range(len(stages))):
            k = turn - place

            @pl.when((k >= 0) & (k < parts))
            def _():
                stages[place](k)

        return carry

    lax.fori_loop(0, parts + len(stages) - 1, advance, 0)

    def finish(k, carry):
        for hop in range(1, bands):
            spread(k, hop).wait_send()
        near_copy(k).wait_send()
        mate_copy(k).wait_send()

        @pl.when(rank == middle - 1)
        def _():
            swap_copy(k).wait_send()

        @pl.when(rank < middle - 1)
        def _():
            line_copy(k).wait_send()

        @pl.when(rank > 0)
        def _():
            back_copy(k).wait_send()

        return carry

    lax.fori_loop(0, parts, finish, 0)
    for k in range(parts):
        write_rows(k, min(128, flat - k * 128)).wait()


def exchange(found, weather, scale, order_local):
    parts, bands, depth, width = found.shape
    buffer = pltpu.VMEM((parts, bands // 2, depth, width), jnp.bfloat16)
    dma = pltpu.SemaphoreType.DMA
    return pl.pallas_call(
        functools.partial(exchange_kernel, order_local),
        out_shape=jax.ShapeDtypeStruct(weather.shape, jnp.bfloat16),
        in_specs=[
            pl.BlockSpec(memory_space=pltpu.VMEM),
            pl.BlockSpec(memory_space=pl.ANY),
            pl.BlockSpec(memory_space=pltpu.SMEM),
        ],
        out_specs=pl.BlockSpec(memory_space=pl.ANY),
        scratch_shapes=[
            pltpu.VMEM((parts, bands, depth, width), jnp.bfloat16),
            buffer,
            buffer,
            buffer,
            buffer,
            pltpu.VMEM((parts, 2, bands // 2, depth, width), jnp.bfloat16),
            pltpu.VMEM((bands * depth, weather.shape[1]), jnp.bfloat16),
            pltpu.VMEM((parts * 128, weather.shape[1]), jnp.bfloat16),
            pltpu.VMEM((128, bands * depth), jnp.bfloat16),
            dma((1,)),
            dma((parts,)),
            dma((parts, bands)),
            dma((parts, bands)),
        ]
        + [dma((parts,))] * 10,
        compiler_params=pltpu.CompilerParams(
            has_side_effects=True, vmem_limit_bytes=60 * 1024 * 1024
        ),
    )(found, weather, scale)


def local(weather, coefficients, channel_scale):
    member_local, channels, rows_local, lon_count = weather.shape
    band_count = lax.axis_size("space")
    order_local = coefficients.shape[3]
    degree_count = coefficients.shape[4]
    order_count = order_local * band_count
    lat_count = rows_local * band_count
    half = round_up(order_local, 32) // 2
    padded = 2 * half

    first_order = lax.axis_index("space") * order_local
    slots = jnp.arange(padded, dtype=jnp.int32)
    orders = first_order + slots
    logs = jnp.pad(diagonal_log(order_count), (0, padded))
    order_logs = lax.dynamic_slice_in_dim(logs, first_order, padded)
    row_first = (lon_count // 2 + 1 - lat_count) // 2
    colatitude = (
        math.pi
        * (row_first + jnp.arange(lat_count, dtype=jnp.int32)).astype(jnp.float32)
        / (lon_count // 2)
    )
    order_values = orders.astype(jnp.float32)[:, None]
    diagonal = jnp.exp(
        order_logs[:, None]
        - 0.5 * math.log(4.0 * math.pi)
        + order_values * jnp.log(jnp.sin(colatitude))[None, :]
    )

    def pair_up(plane):
        return jnp.concatenate([plane[:half], plane[half:]], axis=1)

    order_plane = pair_up(jnp.broadcast_to(order_values, (padded, lat_count)))
    cosine_row = jnp.tile(jnp.cos(colatitude), 2)[None, :]

    turned = coefficients.transpose(0, 1, 3, 2, 4)
    turned = turned.reshape(member_local * channels, order_local, 2, degree_count)
    found = synthesize(turned, order_plane, cosine_row, pair_up(diagonal), rows_local)
    found = found.reshape(found.shape[0], band_count, 4 * half, 128)
    state = weather.reshape(member_local * channels * rows_local, lon_count)
    result = exchange(found, state, jnp.tile(channel_scale, member_local), order_local)
    return result.reshape(weather.shape)


def solution(mesh):
    return jax.shard_map(
        local,
        mesh=mesh,
        in_specs=(P("member", None, "space", None), P("member", None, None, "space", None), P()),
        out_specs=P("member", None, "space", None),
        check_vma=False,
    )
```

```python
import functools
import math

import jax
import jax.numpy as jnp
from jax import lax
from jax.experimental import pallas as pl
from jax.experimental.pallas import tpu as pltpu
from jax.sharding import PartitionSpec as P


def round_up(value, step):
    return (value + step - 1) // step * step


def diagonal_log(order_count):
    steps_up = jnp.arange(1, order_count, dtype=jnp.int32).astype(jnp.float32)
    terms = 0.5 * jnp.log((2.0 * steps_up + 1.0) / (2.0 * steps_up))
    return jnp.concatenate([jnp.zeros((1,), jnp.float32), jnp.cumsum(terms)])


def synthesis_kernel(
    block, lat, order_ref, cosine_ref, diagonal_ref, coef, out_ref, table, kept, held, arrived
):
    half, lanes = order_ref.shape
    channels, order_local, _, degree_count = coef.shape
    rows = held.shape[1]
    both = 2 * rows
    degrees = round_up(degree_count, 8)
    pitch = degrees + 8
    factor = math.sqrt(3.0) * math.sqrt(4.0 * math.pi) / degree_count * 2.0 ** (-30)
    turn = pl.program_id(0)

    def fetch(step, act):
        base = lax.rem(step, 2) * (2 * block)
        for spot in range(2 * block):
            slot = step * block + spot % block + spot // block * half
            slot = jnp.minimum(slot, order_local - 1)
            copy = pltpu.make_async_copy(
                coef.at[:, slot], held.at[base + spot, pl.ds(0, channels)], arrived.at[base + spot]
            )
            act(copy)

    @pl.when(turn == 0)
    def begin():
        fetch(turn, lambda copy: copy.start())

    @pl.when(turn + 1 < pl.num_programs(0))
    def ahead():
        fetch(turn + 1, lambda copy: copy.start())

    @pl.when(pl.program_id(0) == 0)
    def build():
        order = order_ref[...]
        order_square = order * order
        cosine = jnp.broadcast_to(cosine_ref[...], (half, lanes))
        diagonal = diagonal_ref[...]

        def advance(step, carry):
            older, newer, down = carry
            degree = step.astype(jnp.float32)
            wide = jnp.full((half, lanes), degree, jnp.float32)
            square = wide * wide
            ratio = jnp.maximum(square - order_square, 0.25) / jnp.maximum(4.0 * square - 1.0, 1.0)
            up = lax.rsqrt(ratio)
            row = up * (cosine * newer - down * older)
            row = jnp.where(wide < order, 0.0, jnp.where(wide == order, diagonal, row))
            for tile in range(lanes // 128):
                table[pl.ds(tile * half * pitch + step, half, stride=pitch), :] = row[
                    :, tile * 128 : tile * 128 + 128
                ]
            return newer, row, ratio * up

        zero = order * 0.0
        lax.fori_loop(0, degrees, advance, (zero, zero, zero), unroll=4)

    fetch(turn, lambda copy: copy.wait())
    first = turn * block
    low = lax.broadcasted_iota(jnp.int32, (both, lanes), 1) < lanes // 2
    pack = 128 // lat
    bands = lanes // 2 // lat
    groups = out_ref.shape[0]
    deep = half + 8

    def read(spot):
        values = held[lax.rem(turn, 2) * (2 * block) + spot].astype(jnp.float32) * factor
        return values.reshape(both, degree_count).astype(jnp.bfloat16)

    for inner in range(block):
        columns = []
        for tile in range(lanes // 128):
            start = pl.multiple_of((tile * half + first + inner) * pitch, 8)
            columns.append(table[pl.ds(start, degrees), :].astype(jnp.bfloat16))
        values = jnp.concatenate(columns, axis=1)[:degree_count]
        stacked = jnp.concatenate([read(inner), read(inner + block)], axis=0)
        found = jnp.dot(stacked, values, preferred_element_type=jnp.float32)
        merged = jnp.where(low, found[:both], found[both:])
        for tile in range(lanes // 128):
            start = tile * both * deep + first + inner
            kept[pl.ds(start, both, stride=deep), :] = merged[:, tile * 128 : tile * 128 + 128]

    @pl.when(pl.program_id(0) == pl.num_programs(0) - 1)
    def regroup():
        chunk = lax.broadcasted_iota(jnp.int32, (half, 128), 1) // lat
        for tile in range(lanes // 128):
            def one_group(group, carry):
                for part in range(2):
                    planes = []
                    for spot in range(pack):
                        row = tile * both + (group * pack + spot) * 2 + part
                        planes.append(kept[pl.ds(pl.multiple_of(row * deep, 8), half), :])
                    gap = 1
                    while gap < pack:
                        upper = (chunk // gap) % 2 == 1
                        for spot in range(pack):
                            if (spot // gap) % 2 == 0:
                                one, two = planes[spot], planes[spot + gap]
                                planes[spot] = jnp.where(upper, pltpu.roll(two, gap * lat, 1), one)
                                planes[spot + gap] = jnp.where(
                                    upper, two, pltpu.roll(one, 128 - gap * lat, 1)
                                )
                        gap *= 2
                    for spot in range(pack):
                        high, band = divmod(tile * pack + spot, bands)
                        out_ref[group, high, band, part] = planes[spot].astype(jnp.bfloat16)
                return carry

            lax.fori_loop(0, groups, one_group, 0)


def synthesize(coefficients, order_plane, cosine_row, diagonal_plane, lat):
    channels, _, _, degree_count = coefficients.shape
    half, lanes = order_plane.shape
    block = 8
    rows = round_up(channels, 128 // lat)
    out_dims = (rows * lat // 128, 2, lanes // 2 // lat, 2, half, 128)
    return pl.pallas_call(
        functools.partial(synthesis_kernel, block, lat),
        grid=(half // block,),
        out_shape=jax.ShapeDtypeStruct(out_dims, jnp.bfloat16),
        in_specs=[
            pl.BlockSpec((half, lanes), lambda i: (0, 0)),
            pl.BlockSpec((1, lanes), lambda i: (0, 0)),
            pl.BlockSpec((half, lanes), lambda i: (0, 0)),
            pl.BlockSpec(memory_space=pl.ANY),
        ],
        out_specs=pl.BlockSpec(out_dims, lambda i: (0, 0, 0, 0, 0, 0)),
        scratch_shapes=[
            pltpu.VMEM((lanes // 128 * half * (round_up(degree_count, 8) + 8), 128), jnp.float32),
            pltpu.VMEM((lanes // 128 * 2 * rows * (half + 8), 128), jnp.float32),
            pltpu.VMEM((4 * block, rows, 2, degree_count), jnp.int32),
            pltpu.SemaphoreType.DMA((4 * block,)),
        ],
        compiler_params=pltpu.CompilerParams(vmem_limit_bytes=46 * 1024 * 1024),
    )(order_plane, cosine_row, diagonal_plane, coefficients)


def quarter_waves(turns):
    quarter = turns * 4.0
    nearest = jnp.floor(quarter + 0.5)
    angle = (quarter - nearest) * (0.5 * math.pi)
    square = angle * angle
    sine = cosine = None
    for power in (8, 6, 4, 2, 0):
        even = (-1.0) ** (power // 2) / math.factorial(power)
        odd = (-1.0) ** (power // 2) / math.factorial(power + 1)
        cosine = even + (0.0 if cosine is None else cosine * square)
        sine = odd + (0.0 if sine is None else sine * square)
    sine = sine * angle
    half_turns = jnp.floor(nearest * 0.5)
    swap = nearest - 2.0 * half_turns > 0.5
    flip = 1.0 - 2.0 * (half_turns - 2.0 * jnp.floor(half_turns * 0.5))
    one = jnp.where(swap, -sine, cosine) * flip
    two = jnp.where(swap, cosine, sine) * flip
    return one, two


def exchange_kernel(
    order_local, sent, weather, scale, out, raw, near, sums, lower, other, total, basis, field,
    turned, field_in, *sems
):
    a2a_send, a2a_recv = sems[0], sems[1]
    pair = {
        "near": (sems[2], sems[3]),
        "line": (sems[4], sems[5]),
        "swap": (sems[6], sems[7]),
        "back": (sems[8], sems[9]),
        "mate": (sems[10], sems[11]),
    }
    parts, bands, depth, _ = sent.shape
    flat, lon_count = out.shape
    channels = scale.shape[0]
    lat = flat // channels
    member_count = lax.axis_size("member")
    chips = member_count // 2
    middle = chips // 2
    me = lax.axis_index("member")
    space = lax.axis_index("space")
    core = lax.rem(me, 2)
    chip = me // 2
    mate = chip * 2 + 1 - core
    left = chip < middle
    rank = jnp.where(left, chip, chips - 1 - chip)
    inward = jnp.where(left, chip + 1, chip - 1) * 2 + core
    outward = jnp.where(left, chip - 1, chip + 1) * 2 + core
    split = bands // 2
    mesh_ids = pl.DeviceIdType.MESH

    def spread(k, hop):
        target = 0
        bit = 1
        while bit < bands:
            target = target + lax.rem(space // bit + hop // bit, 2) * bit
            bit *= 2
        return pltpu.make_async_remote_copy(
            src_ref=sent.at[k, target],
            dst_ref=raw.at[k, space],
            send_sem=a2a_send.at[k, hop],
            recv_sem=a2a_recv.at[k, hop],
            device_id={"space": target},
            device_id_type=mesh_ids,
        )

    def hand(kind, k, source, landing, target):
        return pltpu.make_async_remote_copy(
            src_ref=source,
            dst_ref=landing,
            send_sem=pair[kind][0].at[k],
            recv_sem=pair[kind][1].at[k],
            device_id={"member": target},
            device_id_type=mesh_ids,
        )

    def near_copy(k):
        return hand("near", k, raw.at[k, pl.ds((1 - core) * split, split)], near.at[k], mate)

    def line_copy(k):
        return hand("line", k, sums.at[k], lower.at[k], inward)

    def swap_copy(k):
        return hand("swap", k, sums.at[k], other.at[k], inward)

    def back_copy(k):
        return hand("back", k, total.at[k, core], total.at[k, core], outward)

    def mate_copy(k):
        return hand("mate", k, total.at[k, core], total.at[k, core], mate)

    def stage_near(k):
        raw[k, space] = sent[k, space]
        for hop in range(1, bands):
            spread(k, hop).wait_recv()
        near_copy(k).start()

    def send_inward(k, level):
        @pl.when(rank == level)
        def _():
            if level == middle - 1:
                swap_copy(k).start()
            else:
                line_copy(k).start()

    def stage_sum(k):
        near_copy(k).wait_recv()
        mine = raw[k, pl.ds(core * split, split)].astype(jnp.float32) + near[k].astype(jnp.float32)
        sums[k] = mine.astype(jnp.bfloat16)
        send_inward(k, 0)

    def stage_line(level, k):
        @pl.when(rank == level)
        def _():
            line_copy(k).wait_recv()
            both = sums[k].astype(jnp.float32) + lower[k].astype(jnp.float32)
            sums[k] = both.astype(jnp.bfloat16)

        send_inward(k, level)

    def send_outward(k, level):
        if level > 0:
            back_copy(k).start()
        mate_copy(k).start()

    def stage_swap(k):
        @pl.when(rank == middle - 1)
        def _():
            swap_copy(k).wait_recv()
            both = sums[k].astype(jnp.float32) + other[k].astype(jnp.float32)
            total[k, core] = both.astype(jnp.bfloat16)
            send_outward(k, middle - 1)

    def stage_back(level, k):
        @pl.when(rank == level)
        def _():
            back_copy(k).wait_recv()
            send_outward(k, level)

    def stage_mate(k):
        mate_copy(k).wait_recv()

    def stage_out(k):
        for which in range(2):
            part = k - 1 + which
            for band in range(bands):
                mean = total[part, band // split, band % split].astype(jnp.float32)
                centred = raw[part, band].astype(jnp.float32) - mean * (1.0 / member_count)
                first = (which * bands + band) * depth
                turned[:, first : first + depth] = centred.T.astype(jnp.bfloat16)
        for start in range(0, lon_count, 256):
            width = min(256, lon_count - start)
            noise = jnp.dot(
                turned[...],
                basis[:, start : start + width],
                preferred_element_type=jnp.float32,
            )
            for step in range(128 // lat):
                channel = k // 2 * (128 // lat) + step

                @pl.when(channel < channels)
                def _():
                    rows = pl.ds(pl.multiple_of(channel * lat, lat), lat)
                    state = field[rows, start : start + width].astype(jnp.float32)
                    state = state + scale[channel] * noise[step * lat : (step + 1) * lat]
                    out[rows, start : start + width] = state.astype(jnp.bfloat16)

    hand_lag, chip_lag = 2, 3
    stages = [(0, stage_near), (hand_lag, stage_sum)]
    lag = hand_lag
    for level in range(1, middle):
        lag += chip_lag
        stages.append((lag, functools.partial(stage_line, level)))
    lag += chip_lag
    stages.append((lag, stage_swap))
    for level in range(middle - 2, -1, -1):
        lag += chip_lag
        stages.append((lag, functools.partial(stage_back, level)))
    lag += hand_lag
    stages.append((lag, stage_mate))

    for k in range(parts):
        for hop in range(1, bands):
            spread(k, hop).start()
    load = pltpu.make_async_copy(weather, field, field_in.at[0])
    load.start()

    half = depth // 2
    lane = lax.broadcasted_iota(jnp.int32, (half, 128), 1).astype(jnp.float32)
    row = lax.broadcasted_iota(jnp.int32, (half, 128), 0).astype(jnp.float32)

    def turns(product):
        rest = product - jnp.floor(product * (1.0 / lon_count)) * lon_count
        rest = jnp.where(rest < 0.0, rest + lon_count, rest)
        rest = jnp.where(rest >= lon_count, rest - lon_count, rest)
        return rest * (1.0 / lon_count)

    def build(index, carry):
        band, high = index // 2, lax.rem(index, 2)
        slot = row + (high * half).astype(jnp.float32)
        order = slot + (band * order_local).astype(jnp.float32)
        weight = jnp.where(order < 0.5, 1.0, math.sqrt(2.0))
        weight = jnp.where(slot < order_local, weight, 0.0)
        real, imag = quarter_waves(turns(order * lane))
        real, imag = weight * real, weight * imag
        turn_real, turn_imag = quarter_waves(turns(order * 128.0))
        first = pl.multiple_of((high * bands + band) * depth, half)
        for start in range(0, lon_count, 128):
            width = min(128, lon_count - start)
            basis[pl.ds(first, half), start : start + width] = real[:, :width].astype(jnp.bfloat16)
            basis[pl.ds(first + half, half), start : start + width] = imag[:, :width].astype(
                jnp.bfloat16
            )
            real, imag = real * turn_real - imag * turn_imag, imag * turn_real + real * turn_imag
        return carry

    lax.fori_loop(0, 2 * bands, build, 0)
    load.wait()

    def advance(turn, carry):
        for wait, stage in reversed(stages):
            k = turn - wait

            @pl.when((k >= 0) & (k < parts))
            def _():
                stage(k)

        k = turn - lag

        @pl.when((k >= 0) & (lax.rem(k, 2) == 1))
        def _():
            stage_out(k)

        return carry

    lax.fori_loop(0, parts + lag, advance, 0)

    def finish(k, carry):
        for hop in range(1, bands):
            spread(k, hop).wait_send()
        near_copy(k).wait_send()
        mate_copy(k).wait_send()

        @pl.when(rank == middle - 1)
        def _():
            swap_copy(k).wait_send()

        @pl.when(rank < middle - 1)
        def _():
            line_copy(k).wait_send()

        @pl.when(rank > 0)
        def _():
            back_copy(k).wait_send()

        return carry

    lax.fori_loop(0, parts, finish, 0)


def exchange(found, weather, scale, order_local):
    parts, bands, depth, width = found.shape
    buffer = pltpu.VMEM((parts, bands // 2, depth, width), jnp.bfloat16)
    dma = pltpu.SemaphoreType.DMA
    return pl.pallas_call(
        functools.partial(exchange_kernel, order_local),
        out_shape=jax.ShapeDtypeStruct(weather.shape, jnp.bfloat16),
        in_specs=[
            pl.BlockSpec(memory_space=pltpu.VMEM),
            pl.BlockSpec(memory_space=pl.ANY),
            pl.BlockSpec(memory_space=pltpu.SMEM),
        ],
        out_specs=pl.BlockSpec(memory_space=pltpu.VMEM),
        scratch_shapes=[
            pltpu.VMEM((parts, bands, depth, width), jnp.bfloat16),
            buffer,
            buffer,
            buffer,
            buffer,
            pltpu.VMEM((parts, 2, bands // 2, depth, width), jnp.bfloat16),
            pltpu.VMEM((2 * bands * depth, weather.shape[1]), jnp.bfloat16),
            pltpu.VMEM(weather.shape, jnp.bfloat16),
            pltpu.VMEM((128, 2 * bands * depth), jnp.bfloat16),
            dma((1,)),
            dma((parts, bands)),
            dma((parts, bands)),
        ]
        + [dma((parts,))] * 10,
        compiler_params=pltpu.CompilerParams(
            has_side_effects=True, vmem_limit_bytes=36 * 1024 * 1024
        ),
        cost_estimate=pl.CostEstimate(
            flops=200 * weather.shape[0] * weather.shape[1] * bands * depth,
            bytes_accessed=4 * weather.shape[0] * weather.shape[1],
            transcendentals=0,
        ),
    )(found, weather, scale)


def local(weather, coefficients, channel_scale):
    member_local, channels, rows_local, lon_count = weather.shape
    band_count = lax.axis_size("space")
    order_local = coefficients.shape[3]
    degree_count = coefficients.shape[4]
    order_count = order_local * band_count
    lat_count = rows_local * band_count
    half = round_up(order_local, 32) // 2
    padded = 2 * half

    first_order = lax.axis_index("space") * order_local
    slots = jnp.arange(padded, dtype=jnp.int32)
    orders = first_order + slots
    logs = jnp.pad(diagonal_log(order_count), (0, padded))
    order_logs = lax.dynamic_slice_in_dim(logs, first_order, padded)
    row_first = (lon_count // 2 + 1 - lat_count) // 2
    colatitude = (
        math.pi
        * (row_first + jnp.arange(lat_count, dtype=jnp.int32)).astype(jnp.float32)
        / (lon_count // 2)
    )
    order_values = orders.astype(jnp.float32)[:, None]
    diagonal = jnp.exp(
        order_logs[:, None]
        - 0.5 * math.log(4.0 * math.pi)
        + order_values * jnp.log(jnp.sin(colatitude))[None, :]
    )

    def pair_up(plane):
        return jnp.concatenate([plane[:half], plane[half:]], axis=1)

    order_plane = pair_up(jnp.broadcast_to(order_values, (padded, lat_count)))
    cosine_row = jnp.tile(jnp.cos(colatitude), 2)[None, :]

    turned = coefficients.transpose(0, 1, 3, 2, 4)
    turned = turned.reshape(member_local * channels, order_local, 2, degree_count)
    found = synthesize(turned, order_plane, cosine_row, pair_up(diagonal), rows_local)
    found = found.reshape(found.shape[0] * 2, band_count, 2 * half, 128)
    state = weather.reshape(member_local * channels * rows_local, lon_count)
    result = exchange(found, state, jnp.tile(channel_scale, member_local), order_local)
    return result.reshape(weather.shape)


def solution(mesh):
    return jax.shard_map(
        local,
        mesh=mesh,
        in_specs=(P("member", None, "space", None), P("member", None, None, "space", None), P()),
        out_specs=P("member", None, "space", None),
        check_vma=False,
    )
```

```python
import functools
import math

import jax
import jax.numpy as jnp
from jax import lax
from jax.experimental import pallas as pl
from jax.experimental.pallas import tpu as pltpu
from jax.sharding import PartitionSpec as P


def round_up(value, step):
    return (value + step - 1) // step * step


def diagonal_log(order_count):
    steps_up = jnp.arange(1, order_count, dtype=jnp.int32).astype(jnp.float32)
    terms = 0.5 * jnp.log((2.0 * steps_up + 1.0) / (2.0 * steps_up))
    return jnp.concatenate([jnp.zeros((1,), jnp.float32), jnp.cumsum(terms)])


def synthesis_kernel(
    block, lat, order_ref, cosine_ref, diagonal_ref, coef, out_ref, table, kept, held, arrived
):
    half, lanes = order_ref.shape
    channels, order_local, _, degree_count = coef.shape
    rows = held.shape[1]
    both = 2 * rows
    degrees = round_up(degree_count, 8)
    pitch = degrees + 8
    factor = math.sqrt(3.0) * math.sqrt(4.0 * math.pi) / degree_count * 2.0 ** (-30)
    turn = pl.program_id(0)

    def fetch(step, act):
        base = lax.rem(step, 2) * (2 * block)
        for spot in range(2 * block):
            slot = step * block + spot % block + spot // block * half
            slot = jnp.minimum(slot, order_local - 1)
            copy = pltpu.make_async_copy(
                coef.at[:, slot], held.at[base + spot, pl.ds(0, channels)], arrived.at[base + spot]
            )
            act(copy)

    @pl.when(turn == 0)
    def begin():
        fetch(turn, lambda copy: copy.start())

    @pl.when(turn + 1 < pl.num_programs(0))
    def ahead():
        fetch(turn + 1, lambda copy: copy.start())

    @pl.when(pl.program_id(0) == 0)
    def build():
        order = order_ref[...]
        order_square = order * order
        cosine = jnp.broadcast_to(cosine_ref[...], (half, lanes))
        diagonal = diagonal_ref[...]

        def advance(step, carry):
            older, newer, down = carry
            degree = step.astype(jnp.float32)
            wide = jnp.full((half, lanes), degree, jnp.float32)
            square = wide * wide
            ratio = jnp.maximum(square - order_square, 0.25) / jnp.maximum(4.0 * square - 1.0, 1.0)
            up = lax.rsqrt(ratio)
            row = up * (cosine * newer - down * older)
            row = jnp.where(wide < order, 0.0, jnp.where(wide == order, diagonal, row))
            for tile in range(lanes // 128):
                table[pl.ds(tile * half * pitch + step, half, stride=pitch), :] = row[
                    :, tile * 128 : tile * 128 + 128
                ]
            return newer, row, ratio * up

        zero = order * 0.0
        lax.fori_loop(0, degrees, advance, (zero, zero, zero), unroll=4)

    fetch(turn, lambda copy: copy.wait())
    first = turn * block
    low = lax.broadcasted_iota(jnp.int32, (both, lanes), 1) < lanes // 2
    pack = 128 // lat
    bands = lanes // 2 // lat
    groups = out_ref.shape[0]
    deep = half + 8

    def read(spot):
        values = held[lax.rem(turn, 2) * (2 * block) + spot].astype(jnp.float32) * factor
        return values.reshape(both, degree_count).astype(jnp.bfloat16)

    for inner in range(block):
        columns = []
        for tile in range(lanes // 128):
            start = pl.multiple_of((tile * half + first + inner) * pitch, 8)
            columns.append(table[pl.ds(start, degrees), :].astype(jnp.bfloat16))
        values = jnp.concatenate(columns, axis=1)[:degree_count]
        stacked = jnp.concatenate([read(inner), read(inner + block)], axis=0)
        found = jnp.dot(stacked, values, preferred_element_type=jnp.float32)
        merged = jnp.where(low, found[:both], found[both:])
        for tile in range(lanes // 128):
            start = tile * both * deep + first + inner
            kept[pl.ds(start, both, stride=deep), :] = merged[:, tile * 128 : tile * 128 + 128]

    @pl.when(pl.program_id(0) == pl.num_programs(0) - 1)
    def regroup():
        chunk = lax.broadcasted_iota(jnp.int32, (half, 128), 1) // lat
        for tile in range(lanes // 128):
            def one_group(group, carry):
                for part in range(2):
                    planes = []
                    for spot in range(pack):
                        row = tile * both + (group * pack + spot) * 2 + part
                        planes.append(kept[pl.ds(pl.multiple_of(row * deep, 8), half), :])
                    gap = 1
                    while gap < pack:
                        upper = (chunk // gap) % 2 == 1
                        for spot in range(pack):
                            if (spot // gap) % 2 == 0:
                                one, two = planes[spot], planes[spot + gap]
                                planes[spot] = jnp.where(upper, pltpu.roll(two, gap * lat, 1), one)
                                planes[spot + gap] = jnp.where(
                                    upper, two, pltpu.roll(one, 128 - gap * lat, 1)
                                )
                        gap *= 2
                    for spot in range(pack):
                        high, band = divmod(tile * pack + spot, bands)
                        out_ref[group, high, band, part] = planes[spot].astype(jnp.bfloat16)
                return carry

            lax.fori_loop(0, groups, one_group, 0)


def synthesize(coefficients, order_plane, cosine_row, diagonal_plane, lat):
    channels, _, _, degree_count = coefficients.shape
    half, lanes = order_plane.shape
    block = 8
    rows = round_up(channels, 128 // lat)
    out_dims = (rows * lat // 128, 2, lanes // 2 // lat, 2, half, 128)
    return pl.pallas_call(
        functools.partial(synthesis_kernel, block, lat),
        grid=(half // block,),
        out_shape=jax.ShapeDtypeStruct(out_dims, jnp.bfloat16),
        in_specs=[
            pl.BlockSpec((half, lanes), lambda i: (0, 0)),
            pl.BlockSpec((1, lanes), lambda i: (0, 0)),
            pl.BlockSpec((half, lanes), lambda i: (0, 0)),
            pl.BlockSpec(memory_space=pl.ANY),
        ],
        out_specs=pl.BlockSpec(out_dims, lambda i: (0, 0, 0, 0, 0, 0)),
        scratch_shapes=[
            pltpu.VMEM((lanes // 128 * half * (round_up(degree_count, 8) + 8), 128), jnp.float32),
            pltpu.VMEM((lanes // 128 * 2 * rows * (half + 8), 128), jnp.float32),
            pltpu.VMEM((4 * block, rows, 2, degree_count), jnp.int32),
            pltpu.SemaphoreType.DMA((4 * block,)),
        ],
        compiler_params=pltpu.CompilerParams(vmem_limit_bytes=46 * 1024 * 1024),
    )(order_plane, cosine_row, diagonal_plane, coefficients)


def quarter_waves(turns):
    quarter = turns * 4.0
    nearest = jnp.floor(quarter + 0.5)
    angle = (quarter - nearest) * (0.5 * math.pi)
    square = angle * angle
    sine = cosine = None
    for power in (8, 6, 4, 2, 0):
        even = (-1.0) ** (power // 2) / math.factorial(power)
        odd = (-1.0) ** (power // 2) / math.factorial(power + 1)
        cosine = even + (0.0 if cosine is None else cosine * square)
        sine = odd + (0.0 if sine is None else sine * square)
    sine = sine * angle
    half_turns = jnp.floor(nearest * 0.5)
    swap = nearest - 2.0 * half_turns > 0.5
    flip = 1.0 - 2.0 * (half_turns - 2.0 * jnp.floor(half_turns * 0.5))
    one = jnp.where(swap, -sine, cosine) * flip
    two = jnp.where(swap, cosine, sine) * flip
    return one, two


def exchange_kernel(
    order_local, sent, weather, scale, out, raw, near, sums, lower, other, total, basis, field,
    turned, field_in, *sems
):
    a2a_send, a2a_recv = sems[0], sems[1]
    pair = {
        "near": (sems[2], sems[3]),
        "line": (sems[4], sems[5]),
        "swap": (sems[6], sems[7]),
        "back": (sems[8], sems[9]),
        "mate": (sems[10], sems[11]),
    }
    parts, bands, depth, _ = sent.shape
    flat, lon_count = out.shape
    channels = scale.shape[0]
    lat = flat // channels
    member_count = lax.axis_size("member")
    chips = member_count // 2
    middle = chips // 2
    me = lax.axis_index("member")
    space = lax.axis_index("space")
    core = lax.rem(me, 2)
    chip = me // 2
    mate = chip * 2 + 1 - core
    left = chip < middle
    rank = jnp.where(left, chip, chips - 1 - chip)
    inward = jnp.where(left, chip + 1, chip - 1) * 2 + core
    outward = jnp.where(left, chip - 1, chip + 1) * 2 + core
    split = bands // 2
    mesh_ids = pl.DeviceIdType.MESH

    def spread(k, hop):
        target = 0
        bit = 1
        while bit < bands:
            target = target + lax.rem(space // bit + hop // bit, 2) * bit
            bit *= 2
        return pltpu.make_async_remote_copy(
            src_ref=sent.at[k, target],
            dst_ref=raw.at[k, space],
            send_sem=a2a_send.at[k, hop],
            recv_sem=a2a_recv.at[k, hop],
            device_id={"space": target},
            device_id_type=mesh_ids,
        )

    def hand(kind, k, source, landing, target):
        return pltpu.make_async_remote_copy(
            src_ref=source,
            dst_ref=landing,
            send_sem=pair[kind][0].at[k],
            recv_sem=pair[kind][1].at[k],
            device_id={"member": target},
            device_id_type=mesh_ids,
        )

    def near_copy(k):
        return hand("near", k, raw.at[k, pl.ds((1 - core) * split, split)], near.at[k], mate)

    def line_copy(k):
        return hand("line", k, sums.at[k], lower.at[k], inward)

    def swap_copy(k):
        return hand("swap", k, sums.at[k], other.at[k], inward)

    def back_copy(k):
        return hand("back", k, total.at[k, core], total.at[k, core], outward)

    def mate_copy(k):
        return hand("mate", k, total.at[k, core], total.at[k, core], mate)

    def stage_near(k):
        raw[k, space] = sent[k, space]
        for hop in range(1, bands):
            spread(k, hop).wait_recv()
        near_copy(k).start()

    def send_inward(k, level):
        @pl.when(rank == level)
        def _():
            if level == middle - 1:
                swap_copy(k).start()
            else:
                line_copy(k).start()

    def stage_sum(k):
        near_copy(k).wait_recv()
        mine = raw[k, pl.ds(core * split, split)].astype(jnp.float32) + near[k].astype(jnp.float32)
        sums[k] = mine.astype(jnp.bfloat16)
        send_inward(k, 0)

    def stage_line(level, k):
        @pl.when(rank == level)
        def _():
            line_copy(k).wait_recv()
            both = sums[k].astype(jnp.float32) + lower[k].astype(jnp.float32)
            sums[k] = both.astype(jnp.bfloat16)

        send_inward(k, level)

    def send_outward(k, level):
        if level > 0:
            back_copy(k).start()
        mate_copy(k).start()

    def stage_swap(k):
        @pl.when(rank == middle - 1)
        def _():
            swap_copy(k).wait_recv()
            both = sums[k].astype(jnp.float32) + other[k].astype(jnp.float32)
            total[k, core] = both.astype(jnp.bfloat16)
            send_outward(k, middle - 1)

    def stage_back(level, k):
        @pl.when(rank == level)
        def _():
            back_copy(k).wait_recv()
            send_outward(k, level)

    def stage_mate(k):
        mate_copy(k).wait_recv()

    def stage_out(k):
        for which in range(2):
            part = k - 1 + which
            for band in range(bands):
                mean = total[part, band // split, band % split].astype(jnp.float32)
                centred = raw[part, band].astype(jnp.float32) - mean * (1.0 / member_count)
                first = (which * bands + band) * depth
                turned[:, first : first + depth] = centred.T.astype(jnp.bfloat16)
        for start in range(0, lon_count, 256):
            width = min(256, lon_count - start)
            noise = jnp.dot(
                turned[...],
                basis[:, start : start + width],
                preferred_element_type=jnp.float32,
            )
            for step in range(128 // lat):
                channel = k // 2 * (128 // lat) + step

                @pl.when(channel < channels)
                def _():
                    rows = pl.ds(pl.multiple_of(channel * lat, lat), lat)
                    state = field[rows, start : start + width].astype(jnp.float32)
                    state = state + scale[channel] * noise[step * lat : (step + 1) * lat]
                    out[rows, start : start + width] = state.astype(jnp.bfloat16)

    hand_lag, chip_lag = 2, 4
    stages = [(0, stage_near), (hand_lag, stage_sum)]
    lag = hand_lag
    for level in range(1, middle):
        lag += chip_lag
        stages.append((lag, functools.partial(stage_line, level)))
    lag += chip_lag
    stages.append((lag, stage_swap))
    for level in range(middle - 2, -1, -1):
        lag += chip_lag
        stages.append((lag, functools.partial(stage_back, level)))
    lag += hand_lag
    stages.append((lag, stage_mate))

    for k in range(parts):
        for hop in range(1, bands):
            spread(k, hop).start()
    load = pltpu.make_async_copy(weather, field, field_in.at[0])
    load.start()

    half = depth // 2
    lane = lax.broadcasted_iota(jnp.int32, (half, 128), 1).astype(jnp.float32)
    row = lax.broadcasted_iota(jnp.int32, (half, 128), 0).astype(jnp.float32)

    def turns(product):
        rest = product - jnp.floor(product * (1.0 / lon_count)) * lon_count
        rest = jnp.where(rest < 0.0, rest + lon_count, rest)
        rest = jnp.where(rest >= lon_count, rest - lon_count, rest)
        return rest * (1.0 / lon_count)

    def build(index, carry):
        band, high = index // 2, lax.rem(index, 2)
        slot = row + (high * half).astype(jnp.float32)
        order = slot + (band * order_local).astype(jnp.float32)
        weight = jnp.where(order < 0.5, 1.0, math.sqrt(2.0))
        weight = jnp.where(slot < order_local, weight, 0.0)
        real, imag = quarter_waves(turns(order * lane))
        real, imag = weight * real, weight * imag
        turn_real, turn_imag = quarter_waves(turns(order * 128.0))
        first = pl.multiple_of((high * bands + band) * depth, half)
        for start in range(0, lon_count, 128):
            width = min(128, lon_count - start)
            basis[pl.ds(first, half), start : start + width] = real[:, :width].astype(jnp.bfloat16)
            basis[pl.ds(first + half, half), start : start + width] = imag[:, :width].astype(
                jnp.bfloat16
            )
            real, imag = real * turn_real - imag * turn_imag, imag * turn_real + real * turn_imag
        return carry

    lax.fori_loop(0, 2 * bands, build, 0)
    load.wait()

    def advance(turn, carry):
        for wait, stage in reversed(stages):
            k = turn - wait

            @pl.when((k >= 0) & (k < parts))
            def _():
                stage(k)

        k = turn - lag

        @pl.when((k >= 0) & (lax.rem(k, 2) == 1))
        def _():
            stage_out(k)

        return carry

    lax.fori_loop(0, parts + lag, advance, 0)

    def finish(k, carry):
        for hop in range(1, bands):
            spread(k, hop).wait_send()
        near_copy(k).wait_send()
        mate_copy(k).wait_send()

        @pl.when(rank == middle - 1)
        def _():
            swap_copy(k).wait_send()

        @pl.when(rank < middle - 1)
        def _():
            line_copy(k).wait_send()

        @pl.when(rank > 0)
        def _():
            back_copy(k).wait_send()

        return carry

    lax.fori_loop(0, parts, finish, 0)


def exchange(found, weather, scale, order_local):
    parts, bands, depth, width = found.shape
    buffer = pltpu.VMEM((parts, bands // 2, depth, width), jnp.bfloat16)
    dma = pltpu.SemaphoreType.DMA
    return pl.pallas_call(
        functools.partial(exchange_kernel, order_local),
        out_shape=jax.ShapeDtypeStruct(weather.shape, jnp.bfloat16),
        in_specs=[
            pl.BlockSpec(memory_space=pltpu.VMEM),
            pl.BlockSpec(memory_space=pl.ANY),
            pl.BlockSpec(memory_space=pltpu.SMEM),
        ],
        out_specs=pl.BlockSpec(memory_space=pltpu.VMEM),
        scratch_shapes=[
            pltpu.VMEM((parts, bands, depth, width), jnp.bfloat16),
            buffer,
            buffer,
            buffer,
            buffer,
            pltpu.VMEM((parts, 2, bands // 2, depth, width), jnp.bfloat16),
            pltpu.VMEM((2 * bands * depth, weather.shape[1]), jnp.bfloat16),
            pltpu.VMEM(weather.shape, jnp.bfloat16),
            pltpu.VMEM((128, 2 * bands * depth), jnp.bfloat16),
            dma((1,)),
            dma((parts, bands)),
            dma((parts, bands)),
        ]
        + [dma((parts,))] * 10,
        compiler_params=pltpu.CompilerParams(
            has_side_effects=True, vmem_limit_bytes=36 * 1024 * 1024
        ),
        cost_estimate=pl.CostEstimate(
            flops=200 * weather.shape[0] * weather.shape[1] * bands * depth,
            bytes_accessed=4 * weather.shape[0] * weather.shape[1],
            transcendentals=0,
        ),
    )(found, weather, scale)


def fused_kernel(
    block, order_ref, cosine_ref, diagonal_ref, coef, weather, levels, out, scale, table, kept, held, sent,
    raw, near, sums, lower, other, total, basis, gathered, turned, arrived, field_in, *sems
):
    a2a_send, a2a_recv = sems[0], sems[1]
    pair = {
        "near": (sems[2], sems[3]),
        "line": (sems[4], sems[5]),
        "swap": (sems[6], sems[7]),
        "back": (sems[8], sems[9]),
        "mate": (sems[10], sems[11]),
    }
    parts, bands, depth, _ = sent.shape
    flat, lon_count = out.shape
    channels, order_local, _, degree_count = coef.shape
    lat = flat // channels
    _, quarter, lanes = order_ref.shape
    half = 2 * quarter
    steps = quarter // block
    groups = parts // 2
    rows = held.shape[1]
    wide = turned.shape[0]
    join = wide // 128
    both = 2 * rows
    degrees = round_up(degree_count, 8)
    pitch = degrees + 8
    pack = 128 // lat
    deep = quarter + 16
    factor = math.sqrt(3.0) * math.sqrt(4.0 * math.pi) / degree_count * 2.0 ** (-30)
    member_count = lax.axis_size("member")
    chips = member_count // 2
    middle = chips // 2
    me = lax.axis_index("member")
    space = lax.axis_index("space")
    core = lax.rem(me, 2)
    chip = me // 2
    mate = chip * 2 + 1 - core
    left = chip < middle
    rank = jnp.where(left, chip, chips - 1 - chip)
    inward = jnp.where(left, chip + 1, chip - 1) * 2 + core
    outward = jnp.where(left, chip - 1, chip + 1) * 2 + core
    split = bands // 2
    mesh_ids = pl.DeviceIdType.MESH

    def partner(hop):
        target = 0
        bit = 1
        while bit < bands:
            target = target + lax.rem(space // bit + hop // bit, 2) * bit
            bit *= 2
        return target

    def spread(k, hop):
        target = partner(hop)
        return pltpu.make_async_remote_copy(
            src_ref=sent.at[k, target],
            dst_ref=raw.at[k, space],
            send_sem=a2a_send.at[k, hop],
            recv_sem=a2a_recv.at[k, hop],
            device_id={"space": target},
            device_id_type=mesh_ids,
        )

    def hand(kind, k, source, landing, target):
        return pltpu.make_async_remote_copy(
            src_ref=source,
            dst_ref=landing,
            send_sem=pair[kind][0].at[k],
            recv_sem=pair[kind][1].at[k],
            device_id={"member": target},
            device_id_type=mesh_ids,
        )

    def near_copy(k):
        return hand("near", k, raw.at[k, pl.ds((1 - core) * split, split)], near.at[k], mate)

    def line_copy(k):
        return hand("line", k, sums.at[k], lower.at[k], inward)

    def swap_copy(k):
        return hand("swap", k, sums.at[k], other.at[k], inward)

    def back_copy(k):
        return hand("back", k, total.at[k, core], total.at[k, core], outward)

    def mate_copy(k):
        return hand("mate", k, total.at[k, core], total.at[k, core], mate)

    def stage_near(k):
        raw[k, space] = sent[k, space]
        for hop in range(1, bands):
            spread(k, hop).wait_recv()
        near_copy(k).start()

    def send_inward(k, level):
        @pl.when(rank == level)
        def _():
            if level == middle - 1:
                swap_copy(k).start()
            else:
                line_copy(k).start()

    def stage_sum(k):
        near_copy(k).wait_recv()
        mine = raw[k, pl.ds(core * split, split)].astype(jnp.float32) + near[k].astype(jnp.float32)
        sums[k] = mine.astype(jnp.bfloat16)
        send_inward(k, 0)

    def stage_line(level, k):
        @pl.when(rank == level)
        def _():
            line_copy(k).wait_recv()
            both = sums[k].astype(jnp.float32) + lower[k].astype(jnp.float32)
            sums[k] = both.astype(jnp.bfloat16)

        send_inward(k, level)

    def send_outward(k, level):
        if level > 0:
            back_copy(k).start()
        mate_copy(k).start()

    def stage_swap(k):
        @pl.when(rank == middle - 1)
        def _():
            swap_copy(k).wait_recv()
            both = sums[k].astype(jnp.float32) + other[k].astype(jnp.float32)
            total[k, core] = both.astype(jnp.bfloat16)
            send_outward(k, middle - 1)

    def stage_back(level, k):
        @pl.when(rank == level)
        def _():
            back_copy(k).wait_recv()
            send_outward(k, level)

    def stage_mate(k):
        mate_copy(k).wait_recv()

    def first_slot(step, side):
        return step // steps * half + lax.rem(step, steps) * block + side * quarter

    def fetch(step, act):
        for side in range(2):
            spot = lax.rem(step, 2) * 2 + side
            start = jnp.minimum(first_slot(step, side), order_local - block)
            copy = pltpu.make_async_copy(
                coef.at[:, pl.ds(start, block)],
                held.at[spot, pl.ds(0, channels)],
                arrived.at[spot],
            )
            act(copy)

    def build_table(which):
        order = order_ref[which]
        order_square = order * order
        cosine = jnp.broadcast_to(cosine_ref[...], (quarter, lanes))
        diagonal = diagonal_ref[which]

        def grow(step, carry):
            older, newer, down = carry
            degree = step.astype(jnp.float32)
            wide = jnp.full((quarter, lanes), degree, jnp.float32)
            square = wide * wide
            ratio = jnp.maximum(square - order_square, 0.25) / jnp.maximum(4.0 * square - 1.0, 1.0)
            up = lax.rsqrt(ratio)
            row = up * (cosine * newer - down * older)
            row = jnp.where(wide < order, 0.0, jnp.where(wide == order, diagonal, row))
            for tile in range(lanes // 128):
                table[pl.ds(tile * quarter * pitch + step, quarter, stride=pitch), :] = row[
                    :, tile * 128 : tile * 128 + 128
                ]
            return newer, row, ratio * up

        zero = order * 0.0
        lax.fori_loop(0, degrees, grow, (zero, zero, zero), unroll=4)

    def synthesize_block(step):
        fetch(step, lambda copy: copy.wait())
        first = lax.rem(step, steps) * block
        low = lax.broadcasted_iota(jnp.int32, (both, lanes), 1) < lanes // 2

        def read(inner, side):
            start = first_slot(step, side)
            place = inner + start - jnp.minimum(start, order_local - block)
            values = held[lax.rem(step, 2) * 2 + side, :, jnp.minimum(place, block - 1)]
            values = (values.astype(jnp.float32) * factor).reshape(both, degree_count)
            return values.astype(jnp.bfloat16)

        for inner in range(block):
            columns = []
            for tile in range(lanes // 128):
                start = pl.multiple_of((tile * quarter + first + inner) * pitch, 8)
                columns.append(table[pl.ds(start, degrees), :].astype(jnp.bfloat16))
            values = jnp.concatenate(columns, axis=1)[:degree_count]
            stacked = jnp.concatenate([read(inner, 0), read(inner, 1)], axis=0)
            found = jnp.dot(stacked, values, preferred_element_type=jnp.float32)
            merged = jnp.where(low, found[:both], found[both:])
            for tile in range(lanes // 128):
                start = tile * both * deep + first + inner
                kept[pl.ds(start, both, stride=deep), :] = merged[:, tile * 128 : tile * 128 + 128]

        @pl.when(step + 2 < 2 * steps)
        def _():
            fetch(step + 2, lambda copy: copy.start())

    def regroup(which):
        chunk = lax.broadcasted_iota(jnp.int32, (quarter, 128), 1) // lat

        def one_group(group, carry):
            for part in range(2):
                found = []
                for tile in range(lanes // 128):
                    planes = []
                    for spot in range(pack):
                        row = tile * both + (group * pack + spot) * 2 + part
                        planes.append(kept[pl.ds(pl.multiple_of(row * deep, 8), quarter), :])
                    gap = 1
                    while gap < pack:
                        upper = (chunk // gap) % 2 == 1
                        for spot in range(pack):
                            if (spot // gap) % 2 == 0:
                                one, two = planes[spot], planes[spot + gap]
                                planes[spot] = jnp.where(upper, pltpu.roll(two, gap * lat, 1), one)
                                planes[spot + gap] = jnp.where(
                                    upper, two, pltpu.roll(one, 128 - gap * lat, 1)
                                )
                        gap *= 2
                    found += planes
                for band in range(bands):
                    plane = jnp.concatenate([found[band], found[bands + band]], axis=0)
                    sent[which * groups + group, band, part * half : (part + 1) * half] = (
                        plane.astype(jnp.bfloat16)
                    )
            return carry

        lax.fori_loop(0, groups, one_group, 0)

    def stage_out(k):
        which = k // groups
        group = lax.rem(k, groups)
        for band in range(bands):
            mean = total[k, band // split, band % split].astype(jnp.float32)
            centred = raw[k, band].astype(jnp.float32) - mean * (1.0 / member_count)
            place = pl.ds(pl.multiple_of(lax.rem(group, join) * 128, 128), 128)
            turned[place, band * depth : (band + 1) * depth] = centred.T.astype(jnp.bfloat16)
        base = group // join * join
        ready = (lax.rem(group, join) == join - 1) | (group == groups - 1)
        first = pl.ds(pl.multiple_of(base * 128, 128), wide)
        orders = pl.ds(pl.multiple_of(which * (bands * depth), 128), bands * depth)

        def product(start, width):
            return jnp.dot(
                turned[...],
                basis[orders, start : start + width],
                preferred_element_type=jnp.float32,
            )

        @pl.when(ready & (which == 0))
        def _():
            for start in range(0, lon_count, 256):
                width = min(256, lon_count - start)
                gathered[first, start : start + width] = product(start, width)

        def emit(count):
            amounts = [scale[base * pack + step] for step in range(count)]
            for start in range(0, lon_count, 256):
                width = min(256, lon_count - start)
                noise = product(start, width) + gathered[first, start : start + width]
                for step in range(count):
                    row = (base * pack + step) * lat
                    span = pl.ds(pl.multiple_of(row, lat), lat)
                    state = out[span, start : start + width].astype(jnp.float32)
                    state = state + amounts[step] * noise[step * lat : (step + 1) * lat]
                    out[span, start : start + width] = state.astype(jnp.bfloat16)

        last = (groups - 1) // join * join

        @pl.when(ready & (which == 1) & (base < last))
        def _():
            emit(join * pack)

        @pl.when(ready & (which == 1) & (base == last))
        def _():
            emit(channels - last * pack)

    hand_lag, chip_lag = 2, 4
    stages = [(0, stage_near), (hand_lag, stage_sum)]
    lag = hand_lag
    for level in range(1, middle):
        lag += chip_lag
        stages.append((lag, functools.partial(stage_line, level)))
    lag += chip_lag
    stages.append((lag, stage_swap))
    for level in range(middle - 2, -1, -1):
        lag += chip_lag
        stages.append((lag, functools.partial(stage_back, level)))
    lag += hand_lag
    stages.append((lag, stage_mate))

    for step in range(2):
        fetch(step, lambda copy: copy.start())

    barrier = pltpu.get_barrier_semaphore()
    for hop in range(1, bands):
        pl.semaphore_signal(
            barrier, inc=1, device_id={"space": partner(hop)}, device_id_type=mesh_ids
        )
    for target in (mate, inward):
        pl.semaphore_signal(barrier, inc=1, device_id={"member": target}, device_id_type=mesh_ids)

    @pl.when(rank > 0)
    def _():
        pl.semaphore_signal(barrier, inc=1, device_id={"member": outward}, device_id_type=mesh_ids)

    build_table(0)

    def low_step(step, carry):
        synthesize_block(step)
        return carry

    lax.fori_loop(0, steps, low_step, 0)
    load = pltpu.make_async_copy(weather, out, field_in.at[0])
    load.start()
    amounts_load = pltpu.make_async_copy(levels, scale, field_in.at[1])
    amounts_load.start()
    regroup(0)

    pl.semaphore_wait(barrier, bands + 1 + jnp.where(rank > 0, 1, 0))

    def fire(k, carry):
        for hop in range(1, bands):
            spread(k, hop).start()
        return carry

    lax.fori_loop(0, groups, fire, 0)
    build_table(1)

    lane = lax.broadcasted_iota(jnp.int32, (half, 128), 1).astype(jnp.float32)
    row = lax.broadcasted_iota(jnp.int32, (half, 128), 0).astype(jnp.float32)

    def turns(product):
        rest = product - jnp.floor(product * (1.0 / lon_count)) * lon_count
        rest = jnp.where(rest < 0.0, rest + lon_count, rest)
        rest = jnp.where(rest >= lon_count, rest - lon_count, rest)
        return rest * (1.0 / lon_count)

    def build_basis(index, carry):
        band, high = index // 2, lax.rem(index, 2)
        slot = row + (high * half).astype(jnp.float32)
        order = slot + (band * order_local).astype(jnp.float32)
        weight = jnp.where(order < 0.5, 1.0, math.sqrt(2.0))
        weight = jnp.where(slot < order_local, weight, 0.0)
        real, imag = quarter_waves(turns(order * lane))
        real, imag = weight * real, weight * imag
        turn_real, turn_imag = quarter_waves(turns(order * 128.0))
        first = pl.multiple_of((high * bands + band) * depth, half)
        for start in range(0, lon_count, 128):
            width = min(128, lon_count - start)
            basis[pl.ds(first, half), start : start + width] = real[:, :width].astype(jnp.bfloat16)
            basis[pl.ds(first + half, half), start : start + width] = imag[:, :width].astype(
                jnp.bfloat16
            )
            real, imag = real * turn_real - imag * turn_imag, imag * turn_real + real * turn_imag
        return carry

    lax.fori_loop(0, 2 * bands, build_basis, 0)
    load.wait()
    amounts_load.wait()

    def advance(turn, carry):
        for wait, stage in reversed(stages):
            k = turn - wait

            @pl.when((k >= 0) & (k < parts))
            def _():
                stage(k)

        @pl.when(turn < steps)
        def _():
            synthesize_block(turn + steps)

        @pl.when(turn == steps - 1)
        def _():
            regroup(1)
            lax.fori_loop(groups, parts, fire, 0)

        k = turn - lag

        @pl.when(k >= 0)
        def _():
            stage_out(k)

        return carry

    lax.fori_loop(0, parts + lag, advance, 0)

    def finish(k, carry):
        for hop in range(1, bands):
            spread(k, hop).wait_send()
        near_copy(k).wait_send()
        mate_copy(k).wait_send()

        @pl.when(rank == middle - 1)
        def _():
            swap_copy(k).wait_send()

        @pl.when(rank < middle - 1)
        def _():
            line_copy(k).wait_send()

        @pl.when(rank > 0)
        def _():
            back_copy(k).wait_send()

        return carry

    lax.fori_loop(0, parts, finish, 0)


def fused_buffers(coefficients, weather, planes, lat):
    channels, _, _, degree_count = coefficients.shape
    _, quarter, lanes = planes
    flat, lon_count = weather.shape
    block = 8
    bands = lanes // 2 // lat
    depth = 4 * quarter
    rows = round_up(channels, 128 // lat)
    parts = 2 * (rows * lat // 128)
    tiles = lanes // 128
    sums = ((parts, bands // 2, depth, 128), jnp.bfloat16)
    return [
        ((tiles * quarter * (round_up(degree_count, 8) + 8), 128), jnp.float32),
        ((tiles * 2 * rows * (quarter + 16), 128), jnp.float32),
        ((4, rows, block, 2, degree_count), jnp.int32),
        ((parts, bands, depth, 128), jnp.bfloat16),
        ((parts, bands, depth, 128), jnp.bfloat16),
        sums,
        sums,
        sums,
        sums,
        ((parts, 2, bands // 2, depth, 128), jnp.bfloat16),
        ((2 * bands * depth, lon_count), jnp.bfloat16),
        ((round_up(parts // 2, 2) * 128, lon_count), jnp.float32),
        ((2 * 128, bands * depth), jnp.bfloat16),
    ]


def fused_fits(buffers, weather):
    sizes = [(dims, kind) for dims, kind in buffers] + [(weather.shape, weather.dtype)]
    bytes_used = sum(
        math.prod(dims[:-1]) * round_up(dims[-1], 128) * jnp.dtype(kind).itemsize
        for dims, kind in sizes
    )
    return bytes_used < 52 * 1024 * 1024


def fused(coefficients, weather, scale, order_planes, cosine_row, diagonal_planes, buffers):
    flat, lon_count = weather.shape
    parts, bands, depth, _ = buffers[3][0]
    block = buffers[2][0][2]
    dma = pltpu.SemaphoreType.DMA
    vmem = pl.BlockSpec(memory_space=pltpu.VMEM)
    hbm = pl.BlockSpec(memory_space=pltpu.HBM)
    return pl.pallas_call(
        functools.partial(fused_kernel, block),
        out_shape=jax.ShapeDtypeStruct(weather.shape, jnp.bfloat16),
        in_specs=[vmem, vmem, vmem, hbm, hbm, hbm],
        out_specs=vmem,
        scratch_shapes=[pltpu.SMEM(scale.shape, jnp.float32)]
        + [pltpu.VMEM(*buffer) for buffer in buffers]
        + [dma((4,)), dma((2,)), dma((parts, bands)), dma((parts, bands))]
        + [dma((parts,))] * 10,
        compiler_params=pltpu.CompilerParams(
            has_side_effects=True, collective_id=0, vmem_limit_bytes=48 * 1024 * 1024
        ),
        cost_estimate=pl.CostEstimate(
            flops=200 * flat * lon_count * bands * depth,
            bytes_accessed=4 * flat * lon_count,
            transcendentals=0,
        ),
    )(order_planes, cosine_row, diagonal_planes, coefficients, weather, scale)


def local(weather, coefficients, channel_scale):
    member_local, channels, rows_local, lon_count = weather.shape
    band_count = lax.axis_size("space")
    order_local = coefficients.shape[3]
    degree_count = coefficients.shape[4]
    order_count = order_local * band_count
    lat_count = rows_local * band_count
    half = round_up(order_local, 32) // 2
    padded = 2 * half

    first_order = lax.axis_index("space") * order_local
    slots = jnp.arange(padded, dtype=jnp.int32)
    orders = first_order + slots
    logs = jnp.pad(diagonal_log(order_count), (0, padded))
    order_logs = lax.dynamic_slice_in_dim(logs, first_order, padded)
    row_first = (lon_count // 2 + 1 - lat_count) // 2
    colatitude = (
        math.pi
        * (row_first + jnp.arange(lat_count, dtype=jnp.int32)).astype(jnp.float32)
        / (lon_count // 2)
    )
    order_values = orders.astype(jnp.float32)[:, None]
    diagonal = jnp.exp(
        order_logs[:, None]
        - 0.5 * math.log(4.0 * math.pi)
        + order_values * jnp.log(jnp.sin(colatitude))[None, :]
    )

    def pair_up(plane):
        return jnp.concatenate([plane[:half], plane[half:]], axis=1)

    order_plane = pair_up(jnp.broadcast_to(order_values, (padded, lat_count)))
    cosine_row = jnp.tile(jnp.cos(colatitude), 2)[None, :]

    turned = coefficients.transpose(0, 1, 3, 2, 4)
    turned = turned.reshape(member_local * channels, order_local, 2, degree_count)
    state = weather.reshape(member_local * channels * rows_local, lon_count)
    scale = jnp.tile(channel_scale, member_local)

    def quarters(plane):
        plane = plane.reshape(2, 2, half // 2, lat_count)
        return jnp.concatenate([plane[:, 0], plane[:, 1]], axis=2)

    buffers = fused_buffers(turned, state, (2, half // 2, 2 * lat_count), rows_local)
    if half % 16 == 0 and fused_fits(buffers, state):
        order_planes = quarters(jnp.broadcast_to(order_values, (padded, lat_count)))
        result = fused(
            turned, state, scale, order_planes, cosine_row, quarters(diagonal), buffers
        )
        return result.reshape(weather.shape)
    found = synthesize(turned, order_plane, cosine_row, pair_up(diagonal), rows_local)
    found = found.reshape(found.shape[0] * 2, band_count, 2 * half, 128)
    result = exchange(found, state, scale, order_local)
    return result.reshape(weather.shape)


def solution(mesh):
    return jax.shard_map(
        local,
        mesh=mesh,
        in_specs=(P("member", None, "space", None), P("member", None, None, "space", None), P()),
        out_specs=P("member", None, "space", None),
        check_vma=False,
    )
```

```python
import functools
import math

import jax
import jax.numpy as jnp
from jax import lax
from jax.experimental import pallas as pl
from jax.experimental.pallas import tpu as pltpu
from jax.sharding import PartitionSpec as P


def round_up(value, step):
    return (value + step - 1) // step * step


def diagonal_log(order_count):
    steps_up = jnp.arange(1, order_count, dtype=jnp.int32).astype(jnp.float32)
    terms = 0.5 * jnp.log((2.0 * steps_up + 1.0) / (2.0 * steps_up))
    return jnp.concatenate([jnp.zeros((1,), jnp.float32), jnp.cumsum(terms)])


def synthesis_kernel(
    block, lat, order_ref, cosine_ref, diagonal_ref, coef, out_ref, table, kept, held, arrived
):
    half, lanes = order_ref.shape
    channels, order_local, _, degree_count = coef.shape
    rows = held.shape[1]
    both = 2 * rows
    degrees = round_up(degree_count, 8)
    pitch = degrees + 8
    factor = math.sqrt(3.0) * math.sqrt(4.0 * math.pi) / degree_count * 2.0 ** (-30)
    turn = pl.program_id(0)

    def fetch(step, act):
        base = lax.rem(step, 2) * (2 * block)
        for spot in range(2 * block):
            slot = step * block + spot % block + spot // block * half
            slot = jnp.minimum(slot, order_local - 1)
            copy = pltpu.make_async_copy(
                coef.at[:, slot], held.at[base + spot, pl.ds(0, channels)], arrived.at[base + spot]
            )
            act(copy)

    @pl.when(turn == 0)
    def begin():
        fetch(turn, lambda copy: copy.start())

    @pl.when(turn + 1 < pl.num_programs(0))
    def ahead():
        fetch(turn + 1, lambda copy: copy.start())

    @pl.when(pl.program_id(0) == 0)
    def build():
        order = order_ref[...]
        order_square = order * order
        cosine = jnp.broadcast_to(cosine_ref[...], (half, lanes))
        diagonal = diagonal_ref[...]

        def advance(step, carry):
            older, newer, down = carry
            degree = step.astype(jnp.float32)
            wide = jnp.full((half, lanes), degree, jnp.float32)
            square = wide * wide
            ratio = jnp.maximum(square - order_square, 0.25) / jnp.maximum(4.0 * square - 1.0, 1.0)
            up = lax.rsqrt(ratio)
            row = up * (cosine * newer - down * older)
            row = jnp.where(wide < order, 0.0, jnp.where(wide == order, diagonal, row))
            for tile in range(lanes // 128):
                table[pl.ds(tile * half * pitch + step, half, stride=pitch), :] = row[
                    :, tile * 128 : tile * 128 + 128
                ]
            return newer, row, ratio * up

        zero = order * 0.0
        lax.fori_loop(0, degrees, advance, (zero, zero, zero), unroll=4)

    fetch(turn, lambda copy: copy.wait())
    first = turn * block
    low = lax.broadcasted_iota(jnp.int32, (both, lanes), 1) < lanes // 2
    pack = 128 // lat
    bands = lanes // 2 // lat
    groups = out_ref.shape[0]
    deep = half + 8

    def read(spot):
        values = held[lax.rem(turn, 2) * (2 * block) + spot].astype(jnp.float32) * factor
        return values.reshape(both, degree_count).astype(jnp.bfloat16)

    for inner in range(block):
        columns = []
        for tile in range(lanes // 128):
            start = pl.multiple_of((tile * half + first + inner) * pitch, 8)
            columns.append(table[pl.ds(start, degrees), :].astype(jnp.bfloat16))
        values = jnp.concatenate(columns, axis=1)[:degree_count]
        stacked = jnp.concatenate([read(inner), read(inner + block)], axis=0)
        found = jnp.dot(stacked, values, preferred_element_type=jnp.float32)
        merged = jnp.where(low, found[:both], found[both:])
        for tile in range(lanes // 128):
            start = tile * both * deep + first + inner
            kept[pl.ds(start, both, stride=deep), :] = merged[:, tile * 128 : tile * 128 + 128]

    @pl.when(pl.program_id(0) == pl.num_programs(0) - 1)
    def regroup():
        chunk = lax.broadcasted_iota(jnp.int32, (half, 128), 1) // lat
        for tile in range(lanes // 128):
            def one_group(group, carry):
                for part in range(2):
                    planes = []
                    for spot in range(pack):
                        row = tile * both + (group * pack + spot) * 2 + part
                        planes.append(kept[pl.ds(pl.multiple_of(row * deep, 8), half), :])
                    gap = 1
                    while gap < pack:
                        upper = (chunk // gap) % 2 == 1
                        for spot in range(pack):
                            if (spot // gap) % 2 == 0:
                                one, two = planes[spot], planes[spot + gap]
                                planes[spot] = jnp.where(upper, pltpu.roll(two, gap * lat, 1), one)
                                planes[spot + gap] = jnp.where(
                                    upper, two, pltpu.roll(one, 128 - gap * lat, 1)
                                )
                        gap *= 2
                    for spot in range(pack):
                        high, band = divmod(tile * pack + spot, bands)
                        out_ref[group, high, band, part] = planes[spot].astype(jnp.bfloat16)
                return carry

            lax.fori_loop(0, groups, one_group, 0)


def synthesize(coefficients, order_plane, cosine_row, diagonal_plane, lat):
    channels, _, _, degree_count = coefficients.shape
    half, lanes = order_plane.shape
    block = 8
    rows = round_up(channels, 128 // lat)
    out_dims = (rows * lat // 128, 2, lanes // 2 // lat, 2, half, 128)
    return pl.pallas_call(
        functools.partial(synthesis_kernel, block, lat),
        grid=(half // block,),
        out_shape=jax.ShapeDtypeStruct(out_dims, jnp.bfloat16),
        in_specs=[
            pl.BlockSpec((half, lanes), lambda i: (0, 0)),
            pl.BlockSpec((1, lanes), lambda i: (0, 0)),
            pl.BlockSpec((half, lanes), lambda i: (0, 0)),
            pl.BlockSpec(memory_space=pl.ANY),
        ],
        out_specs=pl.BlockSpec(out_dims, lambda i: (0, 0, 0, 0, 0, 0)),
        scratch_shapes=[
            pltpu.VMEM((lanes // 128 * half * (round_up(degree_count, 8) + 8), 128), jnp.float32),
            pltpu.VMEM((lanes // 128 * 2 * rows * (half + 8), 128), jnp.float32),
            pltpu.VMEM((4 * block, rows, 2, degree_count), jnp.int32),
            pltpu.SemaphoreType.DMA((4 * block,)),
        ],
        compiler_params=pltpu.CompilerParams(vmem_limit_bytes=46 * 1024 * 1024),
    )(order_plane, cosine_row, diagonal_plane, coefficients)


def quarter_waves(turns):
    quarter = turns * 4.0
    nearest = jnp.floor(quarter + 0.5)
    angle = (quarter - nearest) * (0.5 * math.pi)
    square = angle * angle
    sine = cosine = None
    for power in (8, 6, 4, 2, 0):
        even = (-1.0) ** (power // 2) / math.factorial(power)
        odd = (-1.0) ** (power // 2) / math.factorial(power + 1)
        cosine = even + (0.0 if cosine is None else cosine * square)
        sine = odd + (0.0 if sine is None else sine * square)
    sine = sine * angle
    half_turns = jnp.floor(nearest * 0.5)
    swap = nearest - 2.0 * half_turns > 0.5
    flip = 1.0 - 2.0 * (half_turns - 2.0 * jnp.floor(half_turns * 0.5))
    one = jnp.where(swap, -sine, cosine) * flip
    two = jnp.where(swap, cosine, sine) * flip
    return one, two


def exchange_kernel(
    order_local, sent, weather, scale, out, raw, near, sums, lower, other, total, basis, field,
    turned, field_in, *sems
):
    a2a_send, a2a_recv = sems[0], sems[1]
    pair = {
        "near": (sems[2], sems[3]),
        "line": (sems[4], sems[5]),
        "swap": (sems[6], sems[7]),
        "back": (sems[8], sems[9]),
        "mate": (sems[10], sems[11]),
    }
    parts, bands, depth, _ = sent.shape
    flat, lon_count = out.shape
    channels = scale.shape[0]
    lat = flat // channels
    member_count = lax.axis_size("member")
    chips = member_count // 2
    middle = chips // 2
    me = lax.axis_index("member")
    space = lax.axis_index("space")
    core = lax.rem(me, 2)
    chip = me // 2
    mate = chip * 2 + 1 - core
    left = chip < middle
    rank = jnp.where(left, chip, chips - 1 - chip)
    inward = jnp.where(left, chip + 1, chip - 1) * 2 + core
    outward = jnp.where(left, chip - 1, chip + 1) * 2 + core
    split = bands // 2
    mesh_ids = pl.DeviceIdType.MESH

    def spread(k, hop):
        target = 0
        bit = 1
        while bit < bands:
            target = target + lax.rem(space // bit + hop // bit, 2) * bit
            bit *= 2
        return pltpu.make_async_remote_copy(
            src_ref=sent.at[k, target],
            dst_ref=raw.at[k, space],
            send_sem=a2a_send.at[k, hop],
            recv_sem=a2a_recv.at[k, hop],
            device_id={"space": target},
            device_id_type=mesh_ids,
        )

    def hand(kind, k, source, landing, target):
        return pltpu.make_async_remote_copy(
            src_ref=source,
            dst_ref=landing,
            send_sem=pair[kind][0].at[k],
            recv_sem=pair[kind][1].at[k],
            device_id={"member": target},
            device_id_type=mesh_ids,
        )

    def near_copy(k):
        return hand("near", k, raw.at[k, pl.ds((1 - core) * split, split)], near.at[k], mate)

    def line_copy(k):
        return hand("line", k, sums.at[k], lower.at[k], inward)

    def swap_copy(k):
        return hand("swap", k, sums.at[k], other.at[k], inward)

    def back_copy(k):
        return hand("back", k, total.at[k, core], total.at[k, core], outward)

    def mate_copy(k):
        return hand("mate", k, total.at[k, core], total.at[k, core], mate)

    def stage_near(k):
        raw[k, space] = sent[k, space]
        for hop in range(1, bands):
            spread(k, hop).wait_recv()
        near_copy(k).start()

    def send_inward(k, level):
        @pl.when(rank == level)
        def _():
            if level == middle - 1:
                swap_copy(k).start()
            else:
                line_copy(k).start()

    def stage_sum(k):
        near_copy(k).wait_recv()
        mine = raw[k, pl.ds(core * split, split)].astype(jnp.float32) + near[k].astype(jnp.float32)
        sums[k] = mine.astype(jnp.bfloat16)
        send_inward(k, 0)

    def stage_line(level, k):
        @pl.when(rank == level)
        def _():
            line_copy(k).wait_recv()
            both = sums[k].astype(jnp.float32) + lower[k].astype(jnp.float32)
            sums[k] = both.astype(jnp.bfloat16)

        send_inward(k, level)

    def send_outward(k, level):
        if level > 0:
            back_copy(k).start()
        mate_copy(k).start()

    def stage_swap(k):
        @pl.when(rank == middle - 1)
        def _():
            swap_copy(k).wait_recv()
            both = sums[k].astype(jnp.float32) + other[k].astype(jnp.float32)
            total[k, core] = both.astype(jnp.bfloat16)
            send_outward(k, middle - 1)

    def stage_back(level, k):
        @pl.when(rank == level)
        def _():
            back_copy(k).wait_recv()
            send_outward(k, level)

    def stage_mate(k):
        mate_copy(k).wait_recv()

    def stage_out(k):
        for which in range(2):
            part = k - 1 + which
            for band in range(bands):
                mean = total[part, band // split, band % split].astype(jnp.float32)
                centred = raw[part, band].astype(jnp.float32) - mean * (1.0 / member_count)
                first = (which * bands + band) * depth
                turned[:, first : first + depth] = centred.T.astype(jnp.bfloat16)
        for start in range(0, lon_count, 256):
            width = min(256, lon_count - start)
            noise = jnp.dot(
                turned[...],
                basis[:, start : start + width],
                preferred_element_type=jnp.float32,
            )
            for step in range(128 // lat):
                channel = k // 2 * (128 // lat) + step

                @pl.when(channel < channels)
                def _():
                    rows = pl.ds(pl.multiple_of(channel * lat, lat), lat)
                    state = field[rows, start : start + width].astype(jnp.float32)
                    state = state + scale[channel] * noise[step * lat : (step + 1) * lat]
                    out[rows, start : start + width] = state.astype(jnp.bfloat16)

    hand_lag, chip_lag = 2, 4
    stages = [(0, stage_near), (hand_lag, stage_sum)]
    lag = hand_lag
    for level in range(1, middle):
        lag += chip_lag
        stages.append((lag, functools.partial(stage_line, level)))
    lag += chip_lag
    stages.append((lag, stage_swap))
    for level in range(middle - 2, -1, -1):
        lag += chip_lag
        stages.append((lag, functools.partial(stage_back, level)))
    lag += hand_lag
    stages.append((lag, stage_mate))

    for k in range(parts):
        for hop in range(1, bands):
            spread(k, hop).start()
    load = pltpu.make_async_copy(weather, field, field_in.at[0])
    load.start()

    half = depth // 2
    lane = lax.broadcasted_iota(jnp.int32, (half, 128), 1).astype(jnp.float32)
    row = lax.broadcasted_iota(jnp.int32, (half, 128), 0).astype(jnp.float32)

    def turns(product):
        rest = product - jnp.floor(product * (1.0 / lon_count)) * lon_count
        rest = jnp.where(rest < 0.0, rest + lon_count, rest)
        rest = jnp.where(rest >= lon_count, rest - lon_count, rest)
        return rest * (1.0 / lon_count)

    def build(index, carry):
        band, high = index // 2, lax.rem(index, 2)
        slot = row + (high * half).astype(jnp.float32)
        order = slot + (band * order_local).astype(jnp.float32)
        weight = jnp.where(order < 0.5, 1.0, math.sqrt(2.0))
        weight = jnp.where(slot < order_local, weight, 0.0)
        real, imag = quarter_waves(turns(order * lane))
        real, imag = weight * real, weight * imag
        turn_real, turn_imag = quarter_waves(turns(order * 128.0))
        first = pl.multiple_of((high * bands + band) * depth, half)
        for start in range(0, lon_count, 128):
            width = min(128, lon_count - start)
            basis[pl.ds(first, half), start : start + width] = real[:, :width].astype(jnp.bfloat16)
            basis[pl.ds(first + half, half), start : start + width] = imag[:, :width].astype(
                jnp.bfloat16
            )
            real, imag = real * turn_real - imag * turn_imag, imag * turn_real + real * turn_imag
        return carry

    lax.fori_loop(0, 2 * bands, build, 0)
    load.wait()

    def advance(turn, carry):
        for wait, stage in reversed(stages):
            k = turn - wait

            @pl.when((k >= 0) & (k < parts))
            def _():
                stage(k)

        k = turn - lag

        @pl.when((k >= 0) & (lax.rem(k, 2) == 1))
        def _():
            stage_out(k)

        return carry

    lax.fori_loop(0, parts + lag, advance, 0)

    def finish(k, carry):
        for hop in range(1, bands):
            spread(k, hop).wait_send()
        near_copy(k).wait_send()
        mate_copy(k).wait_send()

        @pl.when(rank == middle - 1)
        def _():
            swap_copy(k).wait_send()

        @pl.when(rank < middle - 1)
        def _():
            line_copy(k).wait_send()

        @pl.when(rank > 0)
        def _():
            back_copy(k).wait_send()

        return carry

    lax.fori_loop(0, parts, finish, 0)


def exchange(found, weather, scale, order_local):
    parts, bands, depth, width = found.shape
    buffer = pltpu.VMEM((parts, bands // 2, depth, width), jnp.bfloat16)
    dma = pltpu.SemaphoreType.DMA
    return pl.pallas_call(
        functools.partial(exchange_kernel, order_local),
        out_shape=jax.ShapeDtypeStruct(weather.shape, jnp.bfloat16),
        in_specs=[
            pl.BlockSpec(memory_space=pltpu.VMEM),
            pl.BlockSpec(memory_space=pl.ANY),
            pl.BlockSpec(memory_space=pltpu.SMEM),
        ],
        out_specs=pl.BlockSpec(memory_space=pltpu.VMEM),
        scratch_shapes=[
            pltpu.VMEM((parts, bands, depth, width), jnp.bfloat16),
            buffer,
            buffer,
            buffer,
            buffer,
            pltpu.VMEM((parts, 2, bands // 2, depth, width), jnp.bfloat16),
            pltpu.VMEM((2 * bands * depth, weather.shape[1]), jnp.bfloat16),
            pltpu.VMEM(weather.shape, jnp.bfloat16),
            pltpu.VMEM((128, 2 * bands * depth), jnp.bfloat16),
            dma((1,)),
            dma((parts, bands)),
            dma((parts, bands)),
        ]
        + [dma((parts,))] * 10,
        compiler_params=pltpu.CompilerParams(
            has_side_effects=True, vmem_limit_bytes=36 * 1024 * 1024
        ),
        cost_estimate=pl.CostEstimate(
            flops=200 * weather.shape[0] * weather.shape[1] * bands * depth,
            bytes_accessed=4 * weather.shape[0] * weather.shape[1],
            transcendentals=0,
        ),
    )(found, weather, scale)


def fused_kernel(
    block, order_ref, cosine_ref, diagonal_ref, coef, weather, levels, out, scale, table, kept, held, sent,
    raw, near, sums, lower, other, total, basis, gathered, turned, arrived, field_in, *sems
):
    a2a_send, a2a_recv = sems[0], sems[1]
    pair = {
        "near": (sems[2], sems[3]),
        "line": (sems[4], sems[5]),
        "swap": (sems[6], sems[7]),
        "back": (sems[8], sems[9]),
        "mate": (sems[10], sems[11]),
    }
    parts, bands, depth, _ = sent.shape
    flat, lon_count = out.shape
    channels, order_local, _, degree_count = coef.shape
    lat = flat // channels
    _, quarter, lanes = order_ref.shape
    half = 2 * quarter
    steps = quarter // block
    groups = parts // 2
    rows = held.shape[1]
    wide = turned.shape[0]
    join = wide // 128
    both = 2 * rows
    degrees = round_up(degree_count, 8)
    pitch = degrees + 8
    pack = 128 // lat
    deep = quarter + 16
    factor = math.sqrt(3.0) * math.sqrt(4.0 * math.pi) / degree_count * 2.0 ** (-30)
    member_count = lax.axis_size("member")
    chips = member_count // 2
    middle = chips // 2
    me = lax.axis_index("member")
    space = lax.axis_index("space")
    core = lax.rem(me, 2)
    chip = me // 2
    mate = chip * 2 + 1 - core
    left = chip < middle
    rank = jnp.where(left, chip, chips - 1 - chip)
    inward = jnp.where(left, chip + 1, chip - 1) * 2 + core
    outward = jnp.where(left, chip - 1, chip + 1) * 2 + core
    split = bands // 2
    mesh_ids = pl.DeviceIdType.MESH

    def partner(hop):
        target = 0
        bit = 1
        while bit < bands:
            target = target + lax.rem(space // bit + hop // bit, 2) * bit
            bit *= 2
        return target

    def spread(k, hop):
        target = partner(hop)
        return pltpu.make_async_remote_copy(
            src_ref=sent.at[k, target],
            dst_ref=raw.at[k, space],
            send_sem=a2a_send.at[k, hop],
            recv_sem=a2a_recv.at[k, hop],
            device_id={"space": target},
            device_id_type=mesh_ids,
        )

    def hand(kind, k, source, landing, target):
        return pltpu.make_async_remote_copy(
            src_ref=source,
            dst_ref=landing,
            send_sem=pair[kind][0].at[k],
            recv_sem=pair[kind][1].at[k],
            device_id={"member": target},
            device_id_type=mesh_ids,
        )

    def near_copy(k):
        return hand("near", k, raw.at[k, pl.ds((1 - core) * split, split)], near.at[k], mate)

    def line_copy(k):
        return hand("line", k, sums.at[k], lower.at[k], inward)

    def swap_copy(k):
        return hand("swap", k, sums.at[k], other.at[k], inward)

    def back_copy(k):
        return hand("back", k, total.at[k, core], total.at[k, core], outward)

    def mate_copy(k):
        return hand("mate", k, total.at[k, core], total.at[k, core], mate)

    def stage_near(k):
        raw[k, space] = sent[k, space]
        for hop in range(1, bands):
            spread(k, hop).wait_recv()
        near_copy(k).start()

    def send_inward(k, level):
        @pl.when(rank == level)
        def _():
            if level == middle - 1:
                swap_copy(k).start()
            else:
                line_copy(k).start()

    def stage_sum(k):
        near_copy(k).wait_recv()
        mine = raw[k, pl.ds(core * split, split)].astype(jnp.float32) + near[k].astype(jnp.float32)
        sums[k] = mine.astype(jnp.bfloat16)
        send_inward(k, 0)

    def stage_line(level, k):
        @pl.when(rank == level)
        def _():
            line_copy(k).wait_recv()
            both = sums[k].astype(jnp.float32) + lower[k].astype(jnp.float32)
            sums[k] = both.astype(jnp.bfloat16)

        send_inward(k, level)

    def send_outward(k, level):
        if level > 0:
            back_copy(k).start()
        mate_copy(k).start()

    def stage_swap(k):
        @pl.when(rank == middle - 1)
        def _():
            swap_copy(k).wait_recv()
            both = sums[k].astype(jnp.float32) + other[k].astype(jnp.float32)
            total[k, core] = both.astype(jnp.bfloat16)
            send_outward(k, middle - 1)

    def stage_back(level, k):
        @pl.when(rank == level)
        def _():
            back_copy(k).wait_recv()
            send_outward(k, level)

    def stage_mate(k):
        mate_copy(k).wait_recv()

    def first_slot(step, side):
        return step // steps * half + lax.rem(step, steps) * block + side * quarter

    def fetch(step, act):
        for side in range(2):
            spot = lax.rem(step, 2) * 2 + side
            start = jnp.minimum(first_slot(step, side), order_local - block)
            copy = pltpu.make_async_copy(
                coef.at[:, pl.ds(start, block)],
                held.at[spot, pl.ds(0, channels)],
                arrived.at[spot],
            )
            act(copy)

    def build_table(which):
        order = order_ref[which]
        order_square = order * order
        cosine = jnp.broadcast_to(cosine_ref[...], (quarter, lanes))
        diagonal = diagonal_ref[which]

        def grow(step, carry):
            older, newer, down = carry
            degree = step.astype(jnp.float32)
            wide = jnp.full((quarter, lanes), degree, jnp.float32)
            square = wide * wide
            ratio = jnp.maximum(square - order_square, 0.25) / jnp.maximum(4.0 * square - 1.0, 1.0)
            up = lax.rsqrt(ratio)
            begin = jnp.where(wide == order, diagonal, 0.0)
            row = (up * cosine) * newer - (up * down * older - begin)
            for tile in range(lanes // 128):
                table[pl.ds(tile * quarter * pitch + step, quarter, stride=pitch), :] = row[
                    :, tile * 128 : tile * 128 + 128
                ]
            return newer, row, ratio * up

        zero = order * 0.0
        lax.fori_loop(0, degrees, grow, (zero, zero, zero), unroll=8)

    def synthesize_block(piece):
        step = piece // 2
        skip = lax.rem(piece, 2) * (block // 2)

        @pl.when(skip == 0)
        def _():
            fetch(step, lambda copy: copy.wait())

        first = lax.rem(step, steps) * block
        low = lax.broadcasted_iota(jnp.int32, (both, lanes), 1) < lanes // 2

        def read(inner, side):
            start = first_slot(step, side)
            place = inner + start - jnp.minimum(start, order_local - block)
            values = held[lax.rem(step, 2) * 2 + side, :, jnp.minimum(place, block - 1)]
            values = (values.astype(jnp.float32) * factor).reshape(both, degree_count)
            return values.astype(jnp.bfloat16)

        for turn in range(block // 2):
            inner = skip + turn
            columns = []
            for tile in range(lanes // 128):
                start = pl.multiple_of((tile * quarter + first + inner) * pitch, 8)
                columns.append(table[pl.ds(start, degrees), :].astype(jnp.bfloat16))
            values = jnp.concatenate(columns, axis=1)[:degree_count]
            stacked = jnp.concatenate([read(inner, 0), read(inner, 1)], axis=0)
            found = jnp.dot(stacked, values, preferred_element_type=jnp.float32)
            merged = jnp.where(low, found[:both], found[both:])
            for tile in range(lanes // 128):
                start = tile * both * deep + first + inner
                kept[pl.ds(start, both, stride=deep), :] = merged[:, tile * 128 : tile * 128 + 128]

        @pl.when((skip > 0) & (step + 2 < 2 * steps))
        def _():
            fetch(step + 2, lambda copy: copy.start())

    def fire(k):
        for hop in range(1, bands):
            spread(k, hop).start()

    def regroup(which):
        chunk = lax.broadcasted_iota(jnp.int32, (quarter, 128), 1) // lat

        def one_group(group, carry):
            for part in range(2):
                found = []
                for tile in range(lanes // 128):
                    planes = []
                    for spot in range(pack):
                        row = tile * both + (group * pack + spot) * 2 + part
                        planes.append(kept[pl.ds(pl.multiple_of(row * deep, 8), quarter), :])
                    gap = 1
                    while gap < pack:
                        upper = (chunk // gap) % 2 == 1
                        for spot in range(pack):
                            if (spot // gap) % 2 == 0:
                                one, two = planes[spot], planes[spot + gap]
                                planes[spot] = jnp.where(upper, pltpu.roll(two, gap * lat, 1), one)
                                planes[spot + gap] = jnp.where(
                                    upper, two, pltpu.roll(one, 128 - gap * lat, 1)
                                )
                        gap *= 2
                    found += planes
                for band in range(bands):
                    plane = jnp.concatenate([found[band], found[bands + band]], axis=0)
                    sent[which * groups + group, band, part * half : (part + 1) * half] = (
                        plane.astype(jnp.bfloat16)
                    )
            @pl.when(group > 0)
            def _():
                fire(which * groups + group - 1)

            return carry

        lax.fori_loop(0, groups, one_group, 0)
        fire(which * groups + groups - 1)

    def stage_out(k):
        which = k // groups
        group = lax.rem(k, groups)
        for band in range(bands):
            mean = total[k, band // split, band % split].astype(jnp.float32)
            centred = raw[k, band].astype(jnp.float32) - mean * (1.0 / member_count)
            place = pl.ds(pl.multiple_of(lax.rem(group, join) * 128, 128), 128)
            turned[place, band * depth : (band + 1) * depth] = centred.T.astype(jnp.bfloat16)
        base = group // join * join
        ready = (lax.rem(group, join) == join - 1) | (group == groups - 1)
        first = pl.ds(pl.multiple_of(base * 128, 128), wide)
        orders = pl.ds(pl.multiple_of(which * (bands * depth), 128), bands * depth)

        def product(start, width):
            return jnp.dot(
                turned[...],
                basis[orders, start : start + width],
                preferred_element_type=jnp.float32,
            )

        @pl.when(ready & (which == 0))
        def _():
            for start in range(0, lon_count, 256):
                width = min(256, lon_count - start)
                gathered[first, start : start + width] = product(start, width)

        def emit(count):
            amounts = [scale[base * pack + step] for step in range(count)]
            for start in range(0, lon_count, 256):
                width = min(256, lon_count - start)
                noise = product(start, width) + gathered[first, start : start + width]
                for step in range(count):
                    row = (base * pack + step) * lat
                    span = pl.ds(pl.multiple_of(row, lat), lat)
                    state = out[span, start : start + width].astype(jnp.float32)
                    state = state + amounts[step] * noise[step * lat : (step + 1) * lat]
                    out[span, start : start + width] = state.astype(jnp.bfloat16)

        last = (groups - 1) // join * join

        @pl.when(ready & (which == 1) & (base < last))
        def _():
            emit(join * pack)

        @pl.when(ready & (which == 1) & (base == last))
        def _():
            emit(channels - last * pack)

    hand_lag, chip_lag = 2, 4
    stages = [(0, stage_near), (hand_lag, stage_sum)]
    lag = hand_lag
    for level in range(1, middle):
        lag += chip_lag
        stages.append((lag, functools.partial(stage_line, level)))
    lag += chip_lag
    stages.append((lag, stage_swap))
    for level in range(middle - 2, -1, -1):
        lag += chip_lag
        stages.append((lag, functools.partial(stage_back, level)))
    lag += hand_lag
    stages.append((lag, stage_mate))

    for step in range(2):
        fetch(step, lambda copy: copy.start())

    barrier = pltpu.get_barrier_semaphore()
    for hop in range(1, bands):
        pl.semaphore_signal(
            barrier, inc=1, device_id={"space": partner(hop)}, device_id_type=mesh_ids
        )
    for target in (mate, inward):
        pl.semaphore_signal(barrier, inc=1, device_id={"member": target}, device_id_type=mesh_ids)

    @pl.when(rank > 0)
    def _():
        pl.semaphore_signal(barrier, inc=1, device_id={"member": outward}, device_id_type=mesh_ids)

    build_table(0)

    def low_step(step, carry):
        synthesize_block(step)
        return carry

    lax.fori_loop(0, 2 * steps, low_step, 0)
    load = pltpu.make_async_copy(weather, out, field_in.at[0])
    load.start()
    amounts_load = pltpu.make_async_copy(levels, scale, field_in.at[1])
    amounts_load.start()
    pl.semaphore_wait(barrier, bands + 1 + jnp.where(rank > 0, 1, 0))
    regroup(0)
    build_table(1)

    lane = lax.broadcasted_iota(jnp.int32, (half, 128), 1).astype(jnp.float32)
    row = lax.broadcasted_iota(jnp.int32, (half, 128), 0).astype(jnp.float32)

    def turns(product):
        rest = product - jnp.floor(product * (1.0 / lon_count)) * lon_count
        rest = jnp.where(rest < 0.0, rest + lon_count, rest)
        rest = jnp.where(rest >= lon_count, rest - lon_count, rest)
        return rest * (1.0 / lon_count)

    def build_basis(index, carry):
        band, high = index // 2, lax.rem(index, 2)
        slot = row + (high * half).astype(jnp.float32)
        order = slot + (band * order_local).astype(jnp.float32)
        weight = jnp.where(order < 0.5, 1.0, math.sqrt(2.0))
        weight = jnp.where(slot < order_local, weight, 0.0)
        real, imag = quarter_waves(turns(order * lane))
        real, imag = weight * real, weight * imag
        turn_real, turn_imag = quarter_waves(turns(order * 128.0))
        first = pl.multiple_of((high * bands + band) * depth, half)
        for start in range(0, lon_count, 128):
            width = min(128, lon_count - start)
            basis[pl.ds(first, half), start : start + width] = real[:, :width].astype(jnp.bfloat16)
            basis[pl.ds(first + half, half), start : start + width] = imag[:, :width].astype(
                jnp.bfloat16
            )
            real, imag = real * turn_real - imag * turn_imag, imag * turn_real + real * turn_imag
        return carry


    def advance(turn, carry):
        for wait, stage in reversed(stages):
            k = turn - wait

            @pl.when((k >= 0) & (k < parts))
            def _():
                stage(k)

        @pl.when(turn < 2 * steps)
        def _():
            synthesize_block(turn + 2 * steps)

        @pl.when(turn == 2 * steps)
        def _():
            regroup(1)

        @pl.when((turn > 2 * steps) & (turn <= 2 * steps + 2 * bands))
        def _():
            build_basis(turn - 2 * steps - 1, 0)

        @pl.when(turn == 2 * steps + 2 * bands + 1)
        def _():
            load.wait()
            amounts_load.wait()

        k = turn - lag

        @pl.when(k >= 0)
        def _():
            stage_out(k)

        return carry

    assert lag > 2 * steps + 2 * bands + 1
    lax.fori_loop(0, parts + lag, advance, 0)

    def finish(k, carry):
        for hop in range(1, bands):
            spread(k, hop).wait_send()
        near_copy(k).wait_send()
        mate_copy(k).wait_send()

        @pl.when(rank == middle - 1)
        def _():
            swap_copy(k).wait_send()

        @pl.when(rank < middle - 1)
        def _():
            line_copy(k).wait_send()

        @pl.when(rank > 0)
        def _():
            back_copy(k).wait_send()

        return carry

    lax.fori_loop(0, parts, finish, 0)


def fused_buffers(coefficients, weather, planes, lat):
    channels, _, _, degree_count = coefficients.shape
    _, quarter, lanes = planes
    flat, lon_count = weather.shape
    block = 8
    bands = lanes // 2 // lat
    depth = 4 * quarter
    rows = round_up(channels, 128 // lat)
    parts = 2 * (rows * lat // 128)
    tiles = lanes // 128
    sums = ((parts, bands // 2, depth, 128), jnp.bfloat16)
    return [
        ((tiles * quarter * (round_up(degree_count, 8) + 8), 128), jnp.float32),
        ((tiles * 2 * rows * (quarter + 16), 128), jnp.float32),
        ((4, rows, block, 2, degree_count), jnp.int32),
        ((parts, bands, depth, 128), jnp.bfloat16),
        ((parts, bands, depth, 128), jnp.bfloat16),
        sums,
        sums,
        sums,
        sums,
        ((parts, 2, bands // 2, depth, 128), jnp.bfloat16),
        ((2 * bands * depth, lon_count), jnp.bfloat16),
        ((round_up(parts // 2, 2) * 128, lon_count), jnp.float32),
        ((2 * 128, bands * depth), jnp.bfloat16),
    ]


def fused_fits(buffers, weather):
    sizes = [(dims, kind) for dims, kind in buffers] + [(weather.shape, weather.dtype)]
    bytes_used = sum(
        math.prod(dims[:-1]) * round_up(dims[-1], 128) * jnp.dtype(kind).itemsize
        for dims, kind in sizes
    )
    return bytes_used < 52 * 1024 * 1024


def fused(coefficients, weather, scale, order_planes, cosine_row, diagonal_planes, buffers):
    flat, lon_count = weather.shape
    parts, bands, depth, _ = buffers[3][0]
    block = buffers[2][0][2]
    dma = pltpu.SemaphoreType.DMA
    vmem = pl.BlockSpec(memory_space=pltpu.VMEM)
    hbm = pl.BlockSpec(memory_space=pltpu.HBM)
    return pl.pallas_call(
        functools.partial(fused_kernel, block),
        out_shape=jax.ShapeDtypeStruct(weather.shape, jnp.bfloat16),
        in_specs=[vmem, vmem, vmem, hbm, hbm, hbm],
        out_specs=vmem,
        scratch_shapes=[pltpu.SMEM(scale.shape, jnp.float32)]
        + [pltpu.VMEM(*buffer) for buffer in buffers]
        + [dma((4,)), dma((2,)), dma((parts, bands)), dma((parts, bands))]
        + [dma((parts,))] * 10,
        compiler_params=pltpu.CompilerParams(
            has_side_effects=True, collective_id=0, vmem_limit_bytes=48 * 1024 * 1024
        ),
        cost_estimate=pl.CostEstimate(
            flops=200 * flat * lon_count * bands * depth,
            bytes_accessed=4 * flat * lon_count,
            transcendentals=0,
        ),
    )(order_planes, cosine_row, diagonal_planes, coefficients, weather, scale)


def local(weather, coefficients, channel_scale):
    member_local, channels, rows_local, lon_count = weather.shape
    band_count = lax.axis_size("space")
    order_local = coefficients.shape[3]
    degree_count = coefficients.shape[4]
    order_count = order_local * band_count
    lat_count = rows_local * band_count
    half = round_up(order_local, 32) // 2
    padded = 2 * half

    first_order = lax.axis_index("space") * order_local
    slots = jnp.arange(padded, dtype=jnp.int32)
    orders = first_order + slots
    logs = jnp.pad(diagonal_log(order_count), (0, padded))
    order_logs = lax.dynamic_slice_in_dim(logs, first_order, padded)
    row_first = (lon_count // 2 + 1 - lat_count) // 2
    colatitude = (
        math.pi
        * (row_first + jnp.arange(lat_count, dtype=jnp.int32)).astype(jnp.float32)
        / (lon_count // 2)
    )
    order_values = orders.astype(jnp.float32)[:, None]
    diagonal = jnp.exp(
        order_logs[:, None]
        - 0.5 * math.log(4.0 * math.pi)
        + order_values * jnp.log(jnp.sin(colatitude))[None, :]
    )

    def pair_up(plane):
        return jnp.concatenate([plane[:half], plane[half:]], axis=1)

    order_plane = pair_up(jnp.broadcast_to(order_values, (padded, lat_count)))
    cosine_row = jnp.tile(jnp.cos(colatitude), 2)[None, :]

    turned = coefficients.transpose(0, 1, 3, 2, 4)
    turned = turned.reshape(member_local * channels, order_local, 2, degree_count)
    state = weather.reshape(member_local * channels * rows_local, lon_count)
    scale = jnp.tile(channel_scale, member_local)

    buffers = fused_buffers(turned, state, (2, half // 2, 2 * lat_count), rows_local)
    if half % 16 == 0 and fused_fits(buffers, state):
        quarter = half // 2
        dims = (2, quarter, 2 * lat_count)
        lane = lax.broadcasted_iota(jnp.int32, dims, 2)
        low = lane < lat_count
        slot = lax.broadcasted_iota(jnp.int32, dims, 0) * half
        slot = slot + lax.broadcasted_iota(jnp.int32, dims, 1) + jnp.where(low, 0, quarter)
        order_planes = (first_order + slot).astype(jnp.float32)

        def angles(lane):
            return math.pi * (row_first + lane % lat_count).astype(jnp.float32) / (lon_count // 2)

        logs_wide = order_logs.reshape(2, 2, quarter, 1)
        logs_wide = jnp.where(low, logs_wide[:, 0], logs_wide[:, 1])
        diagonal_planes = jnp.exp(
            logs_wide
            - 0.5 * math.log(4.0 * math.pi)
            + order_planes * jnp.log(jnp.sin(angles(lane)))
        )
        cosine_wide = jnp.cos(angles(lax.broadcasted_iota(jnp.int32, (1, 2 * lat_count), 1)))
        result = fused(turned, state, scale, order_planes, cosine_wide, diagonal_planes, buffers)
        return result.reshape(weather.shape)
    found = synthesize(turned, order_plane, cosine_row, pair_up(diagonal), rows_local)
    found = found.reshape(found.shape[0] * 2, band_count, 2 * half, 128)
    result = exchange(found, state, scale, order_local)
    return result.reshape(weather.shape)


def solution(mesh):
    return jax.shard_map(
        local,
        mesh=mesh,
        in_specs=(P("member", None, "space", None), P("member", None, None, "space", None), P()),
        out_specs=P("member", None, "space", None),
        check_vma=False,
    )
```
